128 devices in a mesh: batch: 1, t: 128 (over z, y, x, core).
Axes of the slice: x: 4, y: 4, z: 4, core: 2. Of those that a mesh axis runs over, the one named last changes fastest.
Arguments:
- z: bfloat16 [256, 16, 96, 128], P(('batch', 't'))
- w: bfloat16 [5, 3, 3, 3, 128, 128], replicated
- b: float32 [5, 128], replicated
- gamma: float32 [4, 128], replicated
- beta: float32 [4, 128], replicated
Outputs:
- output: bfloat16 [512, 32, 192, 128], P(('batch', 't'))
All inputs are finite; a program needn't handle non-finite values.
Results may differ from the reference program's by a relative error of at most 0.0145726.
Values are sent between devices in bfloat16 or wider.
A program may use at most 1 GiB of HBM per device.

```python
import jax
import jax.numpy as jnp
from jax import lax

T = 256
H = 16
W = 96
C = 128
GROUPS = 32
EPS = 1e-6
DN = ('NDHWC', 'DHWIO', 'NDHWC')


def setup_inputs(seed: int = 0, part: int = 0) -> dict:
    key = jax.random.key(seed)
    kz, ka, km = jax.random.split(jax.random.fold_in(key, part), 3)
    kw, kb, kg, kbe = jax.random.split(key, 4)
    amp = jnp.exp(0.5 * jax.random.normal(ka, (T, 1, 1, 1), jnp.float32))
    ramp = jnp.linspace(-1.0, 1.0, T)[:, None, None, None]
    mean = ramp * jax.random.normal(km, (1, 1, 1, C), jnp.float32)
    z = amp * jax.random.normal(kz, (T, H, W, C), jnp.float32) + mean
    w = jax.random.normal(kw, (5, 3, 3, 3, C, C), jnp.float32) * (27 * C) ** -0.5
    b = 0.1 * jax.random.normal(kb, (5, C), jnp.float32)
    gamma = 1.0 + 0.2 * jax.random.normal(kg, (4, C), jnp.float32)
    beta = 0.2 * jax.random.normal(kbe, (4, C), jnp.float32)
    return {'z': z.astype(jnp.bfloat16), 'w': w.astype(jnp.bfloat16), 'b': b, 'gamma': gamma, 'beta': beta}


def _conv(x, wk, bk):
    xp = jnp.concatenate([x[:1], x[:1], x], axis=0).astype(jnp.float32)
    y = lax.conv_general_dilated(xp[None], wk.astype(jnp.float32), (1, 1, 1), ((0, 0), (1, 1), (1, 1)), dimension_numbers=DN)[0]
    return (y + bk).astype(jnp.bfloat16)


def _norm_act(x, g, be):
    xf = x.astype(jnp.float32).reshape(x.shape[:-1] + (GROUPS, x.shape[-1] // GROUPS))
    cnt = xf.size // GROUPS
    mean = jnp.sum(xf, axis=(0, 1, 2, 4)) / cnt
    var = jnp.sum(xf * xf, axis=(0, 1, 2, 4)) / cnt - mean * mean
    xn = ((xf - mean[:, None]) * lax.rsqrt(var + EPS)[:, None]).reshape(x.shape) * g + be
    xn = xn.astype(jnp.bfloat16).astype(jnp.float32)
    return jax.nn.silu(xn).astype(jnp.bfloat16)


def _resblock(x, w, b, gamma, beta, i, j):
    h = _conv(_norm_act(x, gamma[i], beta[i]), w[j], b[j])
    h = _conv(_norm_act(h, gamma[i + 1], beta[i + 1]), w[j + 1], b[j + 1])
    return (x.astype(jnp.float32) + h.astype(jnp.float32)).astype(jnp.bfloat16)


def _upsample(x):
    x = jnp.repeat(jnp.repeat(x, 2, axis=1), 2, axis=2)
    return jnp.concatenate([x[:1], jnp.repeat(x[1:], 2, axis=0)], axis=0)


def reference(z, w, b, gamma, beta):
    x = _resblock(z, w, b, gamma, beta, 0, 0)
    u = _conv(_upsample(x), w[2], b[2])
    y = _resblock(u, w, b, gamma, beta, 2, 3)
    return jnp.concatenate([y[:1], y], axis=0)
```

```python
import functools

import jax
import jax.numpy as jnp
import numpy as np
from jax import lax
from jax.experimental import pallas as pl
from jax.experimental.pallas import tpu as pltpu
from jax.sharding import PartitionSpec as P

F32, BF = jnp.float32, jnp.bfloat16
EPS = 1e-6
C = 128
MESH = pl.DeviceIdType.MESH
VMEM_LIMIT = 60 * 2**20


def vmem():
    return pl.BlockSpec(memory_space=pltpu.VMEM)


def dup(v):
    return jnp.concatenate([v, v], axis=1)


def all_reduce(parts, groups, cid):
    ns = len(groups)
    strides = [int(np.prod(groups[:i])) for i in range(ns)]
    np_ = len(parts)

    def kern(*refs):
        s_refs, o_ref = refs[:np_], refs[np_]
        rest = refs[np_ + 1:]
        slots, cur, ssem, rsem = rest[:ns], rest[ns], rest[ns + 1], rest[ns + 2]
        me = lax.axis_index('t')
        bar = pltpu.get_barrier_semaphore()

        def peer(i, g, st):
            d = lax.rem(lax.div(me, st), g)
            return me + (lax.rem(d + i, g) - d) * st, d

        for g, st in zip(groups, strides):
            for i in range(1, g):
                pl.semaphore_signal(bar, inc=1, device_id={'t': peer(i, g, st)[0]}, device_id_type=MESH)
        v = s_refs[0][...]
        for s in s_refs[1:]:
            v = v + s[...]
        cur[0] = v
        pl.semaphore_wait(bar, sum(g - 1 for g in groups))
        for k, (g, st) in enumerate(zip(groups, strides)):
            if k:
                cur[k] = v
            d = lax.rem(lax.div(me, st), g)
            slots[k][pl.ds(d, 1)] = v[None]
            for i in range(1, g):
                pltpu.make_async_remote_copy(cur.at[k], slots[k].at[d], ssem.at[k], rsem.at[k], device_id={'t': peer(i, g, st)[0]}, device_id_type=MESH).start()
            w = slots[k].at[pl.ds(0, g - 1)]
            pltpu.make_async_copy(w, w, rsem.at[k]).wait()
            v = jnp.sum(slots[k][...], axis=0)
        o_ref[...] = v
        for k, g in enumerate(groups):
            w = slots[k].at[pl.ds(0, g - 1)]
            pltpu.make_async_copy(w, w, ssem.at[k]).wait()

    return pl.pallas_call(
        kern, out_shape=jax.ShapeDtypeStruct((2, C), F32), in_specs=[vmem()] * np_, out_specs=vmem(),
        scratch_shapes=[pltpu.VMEM((g, 2, C), F32) for g in groups] + [pltpu.VMEM((ns, 2, C), F32), pltpu.SemaphoreType.DMA((ns,)), pltpu.SemaphoreType.DMA((ns,))],
        compiler_params=pltpu.CompilerParams(collective_id=cid, has_side_effects=True), name='sum_stats')(*parts)


def group_sum(s):
    lane = lax.broadcasted_iota(jnp.int32, s.shape, 1) % 4
    out = s
    for k in (1, 2, 3):
        up = pltpu.roll(s, C - k, 1)
        dn = pltpu.roll(s, 4 - k, 1)
        out = out + jnp.where(lane + k < 4, up, dn)
    return out


def norm_rows(s, cnt):
    s = group_sum(s)
    mean = s[0:1] / cnt
    return mean, lax.rsqrt(s[1:2] / cnt - mean * mean + EPS)


def act(x, mean, inv, g, be):
    v = (((x.astype(F32) - mean) * inv) * g + be).astype(BF).astype(F32)
    return v * jax.nn.sigmoid(v)


def shift(v, by):
    n = v.shape[0]
    row = lax.broadcasted_iota(jnp.int32, v.shape, 0)
    return jnp.where(row == (0 if by > 0 else n - 1), 0.0, pltpu.roll(v, by % n, 0))


def stats_of(h):
    hf = h.astype(F32)
    return jnp.sum(hf, axis=0, keepdims=True), jnp.sum(hf * hf, axis=0, keepdims=True)


def cost(flops):
    return pl.CostEstimate(flops=int(flops), bytes_accessed=int(8e6), transcendentals=0)


def z_stats(z):
    n, hh, ww, _ = z.shape

    def kern(z_ref, o_ref):
        o_ref[...] = jnp.zeros_like(o_ref)

        def body(i, c):
            s1, s2 = stats_of(z_ref[i // hh, i % hh])
            return c[0] + s1, c[1] + s2
        zero = jnp.zeros((1, C), F32)
        s1, s2 = lax.fori_loop(0, n * hh, body, (zero, zero))
        o_ref[0:1] = s1
        o_ref[1:2] = s2

    return pl.pallas_call(kern, out_shape=jax.ShapeDtypeStruct((2, C), F32), in_specs=[vmem()], out_specs=vmem(), cost_estimate=cost(1e7), name='z_stats')(z)


def conv_a(x, halo, s, g, be, w, b, cnt, res=None, R=8):
    n, hh, ww, _ = x.shape

    def kern(*refs):
        if res is None:
            x_ref, halo_ref, s_ref, g_ref, be_ref, w_ref, b_ref, o_ref, st_ref, A, W = refs
        else:
            x_ref, halo_ref, s_ref, g_ref, be_ref, w_ref, b_ref, res_ref, o_ref, A, W = refs
        first = lax.axis_index('t') == 0
        for q in range(4):
            for di in range(3):
                for dj in range(3):
                    t = di * 3 + dj
                    rows = pl.ds(dj * C, C)
                    W[q * 3 + di, rows, 0:C] = w_ref[q * 9 + t] if q < 3 else jnp.zeros((C, C), BF)
                    W[q * 3 + di, rows, C:2 * C] = w_ref[(q - 1) * 9 + t] if q > 0 else jnp.zeros((C, C), BF)
        mean, inv = norm_rows(s_ref[...], cnt)
        gg, bb = g_ref[...], be_ref[...]
        for q in range(4):
            A[q, 0] = jnp.zeros((ww, 3 * C), BF)
            A[q, hh + 1] = jnp.zeros((ww, 3 * C), BF)

            def arow(r, c):
                v = x_ref[q - 2, r] if q >= 2 else jnp.where(first, x_ref[0, r], halo_ref[q, r])
                v = act(v, mean, inv, gg, bb)
                A[q, r + 1, :, C:2 * C] = v.astype(BF)
                A[q, r + 1, :, 0:C] = shift(v, 1).astype(BF)
                A[q, r + 1, :, 2 * C:] = shift(v, -1).astype(BF)
                return c
            lax.fori_loop(0, hh, arow, 0, unroll=2)
        bias = dup(b_ref[...])
        t1 = t2 = jnp.zeros((1, C), F32)
        for rc in range(hh // R):
            r0 = rc * R
            parts = [A[q, pl.ds(r0 + di, R)].reshape(R * ww, 3 * C) for q in range(4) for di in range(3)]
            acc = jnp.dot(jnp.concatenate(parts, axis=1), W[...].reshape(12 * 3 * C, 2 * C), preferred_element_type=F32)
            h = (acc + bias).astype(BF)
            for f in range(2):
                hf = h[:, f * C:(f + 1) * C].reshape(R, ww, C)
                if res is None:
                    o_ref[f, pl.ds(r0, R)] = hf
                else:
                    o_ref[f, pl.ds(r0, R)] = (res_ref[f, pl.ds(r0, R)].astype(F32) + hf.astype(F32)).astype(BF)
            if res is None:
                s1, s2 = stats_of(h)
                t1 = t1 + (s1[:, :C] + s1[:, C:])
                t2 = t2 + (s2[:, :C] + s2[:, C:])
        if res is None:
            st_ref[0:1] = t1
            st_ref[1:2] = t2

    shp = jax.ShapeDtypeStruct(x.shape, BF)
    args = (x, halo, s, g, be, w, b) + (() if res is None else (res,))
    return pl.pallas_call(
        kern, in_specs=[vmem()] * len(args), out_specs=[vmem(), vmem()] if res is None else vmem(),
        out_shape=[shp, jax.ShapeDtypeStruct((2, C), F32)] if res is None else shp,
        scratch_shapes=[pltpu.VMEM((4, hh + 2, ww, 3 * C), BF), pltpu.VMEM((12, 3 * C, 2 * C), BF)],
        compiler_params=pltpu.CompilerParams(vmem_limit_bytes=VMEM_LIMIT), cost_estimate=cost(7e9), name='conv_a')(*args)


def up_conv(x, halo, w, b):
    n, hh, ww, _ = x.shape
    wp = ww + 16
    nq = n + 2

    def kern(x_ref, halo_ref, w_ref, b_ref, o_ref, st_ref, X, Wpp, Wpc, Wcp, Wcc, PP, PC, CP, CC, Q):
        first = lax.axis_index('t') == 0

        def kk(t, di, dj):
            return w_ref[t * 9 + di * 3 + dj]

        z = jnp.zeros((C, C), BF)

        def put(W, k, di, dj):
            for ti in range(2):
                W[ti, pl.ds(k * C, C), 0:C] = kk(0 if ti == 0 else 2, di, dj)
                W[ti, pl.ds(k * C, C), C:2 * C] = z if ti == 0 else kk(1, di, dj)
        for k, (di, dj) in enumerate(((0, 0), (0, 2), (2, 0), (2, 2))):
            put(Wpp, k, di, dj)
        for k, di in enumerate((0, 2)):
            put(Wpc, k, di, 1)
        for k, dj in enumerate((0, 2)):
            put(Wcp, k, 1, dj)
        put(Wcc, 0, 1, 1)

        for q in range(nq):
            X[q, 0] = jnp.zeros((wp, 2 * C), BF)
            X[q, hh + 1] = jnp.zeros((wp, 2 * C), BF)

            def xrow(r, c):
                v = x_ref[q - 2, r] if q >= 2 else jnp.where(first, x_ref[0, r], halo_ref[q, r])
                X[q, r + 1, 0:ww, C:2 * C] = v
                X[q, r + 1, ww:wp, C:2 * C] = jnp.zeros((16, C), BF)
                vf = v.astype(F32)
                X[q, r + 1, 0:ww, 0:C] = shift(vf, 1).astype(BF)
                tail = jnp.where(lax.broadcasted_iota(jnp.int32, (16, C), 0) == 0, vf[ww - 1:ww], 0.0)
                X[q, r + 1, ww:wp, 0:C] = tail.astype(BF)
                return c
            lax.fori_loop(0, hh, xrow, 0, unroll=2)

        bias = b_ref[...]
        t1 = t2 = jnp.zeros((1, C), F32)
        for q in range(nq):
            frames = (q - 1, q) if q else (q,)
            tis = (0, 1) if q else (1,)

            def taps(rows, r0, nr, cols):
                parts = [X[f, pl.ds(r0 + dr, nr), 0:(wp if cols == 0 else ww), cols:2 * C].reshape(-1, 2 * C - cols) for f in frames for dr in rows]
                return jnp.concatenate(parts, axis=1) if len(parts) > 1 else parts[0]

            def wt(W):
                k = W.shape[1]
                return W[...].reshape(2 * k, 2 * C) if q else W[1]

            half = hh // 2
            for i0, nr in ((0, half), (half, half + 1)):
                PP[pl.ds(i0, nr)] = jnp.dot(taps((0, 1), i0, nr, 0), wt(Wpp), preferred_element_type=F32).reshape(nr, wp, 2 * C)
                PC[pl.ds(i0, nr)] = jnp.dot(taps((0, 1), i0, nr, C), wt(Wpc), preferred_element_type=F32).reshape(nr, ww, 2 * C)
            for i0 in (0, half):
                CP[pl.ds(i0, half)] = jnp.dot(taps((1,), i0, half, 0), wt(Wcp), preferred_element_type=F32).reshape(half, wp, 2 * C)
                CC[pl.ds(i0, half)] = jnp.dot(taps((1,), i0, half, C), wt(Wcc), preferred_element_type=F32).reshape(half, ww, 2 * C)

            def comb(i, carry):
                a1, a2, b1, b2 = carry
                cp, cc = CP[i], CC[i]
                for pr in range(2):
                    fp = PP[i + pr] + cp
                    fc = PC[i + pr] + cc
                    for pc in range(2):
                        v = (fp[0:ww] if pc == 0 else pltpu.roll(fp, wp - 1, 0)[0:ww]) + fc
                        if q:
                            ev = (v[:, :C] + Q[pr, pc, i]) + bias
                            od = (v[:, :C] + v[:, C:]) + bias
                            ev, od = ev.astype(BF), od.astype(BF)
                            o_ref[2 * q - 2, 2 * i + pr, :, pc * C:(pc + 1) * C] = ev
                            o_ref[2 * q - 1, 2 * i + pr, :, pc * C:(pc + 1) * C] = od
                            if q >= 2:
                                e1, e2 = stats_of(ev)
                                d1, d2 = stats_of(od)
                                a1, a2, b1, b2 = a1 + e1, a2 + e2, b1 + d1, b2 + d2
                        if q < nq - 1:
                            Q[pr, pc, i] = v[:, C:]
                return a1, a2, b1, b2

            zero = jnp.zeros((1, C), F32)
            a1, a2, b1, b2 = lax.fori_loop(0, hh, comb, (zero,) * 4)
            if q == 2:
                a1 = jnp.where(first, 0.0, a1)
                a2 = jnp.where(first, 0.0, a2)
            t1 = t1 + a1 + b1
            t2 = t2 + a2 + b2
        st_ref[0:1] = t1
        st_ref[1:2] = t2

    return pl.pallas_call(
        kern, in_specs=[vmem()] * 4, out_specs=[vmem(), vmem()],
        out_shape=[jax.ShapeDtypeStruct((2 * n + 2, 2 * hh, ww, 2 * C), BF), jax.ShapeDtypeStruct((2, C), F32)],
        scratch_shapes=[pltpu.VMEM((nq, hh + 2, wp, 2 * C), BF)]
        + [pltpu.VMEM((2, k * C, 2 * C), BF) for k in (4, 2, 2, 1)]
        + [pltpu.VMEM((hh + 1, wp, 2 * C), F32), pltpu.VMEM((hh + 1, ww, 2 * C), F32), pltpu.VMEM((hh, wp, 2 * C), F32), pltpu.VMEM((hh, ww, 2 * C), F32), pltpu.VMEM((2, 2, hh, ww, C), F32)],
        compiler_params=pltpu.CompilerParams(vmem_limit_bytes=VMEM_LIMIT), cost_estimate=cost(1e10), name='up_conv')(x, halo, w, b)


def build_wb(w_ref, W):
    W[...] = jnp.zeros_like(W)
    for t in range(9):
        for d in range(3):
            k = w_ref[t * 3 + d]
            W[t, pl.ds(d * C, C), 0:C] = k
            W[t, pl.ds((d + 1) * C, C), C:2 * C] = k


def conv_b(ins, s, g, be, w, b, cnt, out_from, nf, weight0=False, fin=None, halo=False, R=8):
    _, hh, wh, _ = ins[0][0].shape
    ni = len(ins)
    ring = 3

    def kern(*refs):
        x_refs = refs[:ni]
        s_ref, g_ref, be_ref, w_ref, b_ref = refs[ni:ni + 5]
        rest = refs[ni + 5:]
        if fin is None:
            o_ref, st_ref, A, W = rest
        else:
            u_ref = rest[0]
            o_ref, A, W, T = rest[-4:]
        step = pl.program_id(0)
        first = lax.axis_index('t') == 0

        @pl.when(step == 0)
        def _():
            build_wb(w_ref, W)
            for k in range(ring):
                A[k, 0] = jnp.zeros((wh, 4 * C), BF)
                A[k, hh + 1] = jnp.zeros((wh, 4 * C), BF)
            if fin is None:
                st_ref[...] = jnp.zeros_like(st_ref)
        slot = lax.rem(step, ring)
        mean, inv = norm_rows(s_ref[...], cnt)
        mean, inv, gg, bb = dup(mean), dup(inv), dup(g_ref[...]), dup(be_ref[...])

        def fill(x_ref):
            def arow(r, c):
                v = act(x_ref[0, r], mean, inv, gg, bb)
                A[slot, r + 1, :, C:3 * C] = v.astype(BF)
                A[slot, r + 1, :, 0:C] = shift(v[:, C:], 1).astype(BF)
                A[slot, r + 1, :, 3 * C:] = shift(v[:, :C], -1).astype(BF)
                return c
            lax.fori_loop(0, hh, arow, 0, unroll=4)
        if ni == 1:
            fill(x_refs[0])
        else:
            use_halo = jnp.logical_and(step < 2, jnp.logical_not(first)) if halo else step < 2

            @pl.when(use_halo)
            def _():
                fill(x_refs[0])

            @pl.when(jnp.logical_not(use_halo))
            def _():
                fill(x_refs[1])

        @pl.when(step >= 2)
        def _():
            bias = dup(b_ref[...])
            t1 = t2 = jnp.zeros((1, C), F32)
            for rc in range(hh // R):
                r0 = rc * R
                parts = []
                for k in range(3):
                    sl = lax.rem(step + 1 + k, ring)
                    for di in range(3):
                        parts.append(A[sl, pl.ds(r0 + di, R)].reshape(R * wh, 4 * C))
                acc = jnp.dot(jnp.concatenate(parts, axis=1), W[...].reshape(36 * C, 2 * C), preferred_element_type=F32)
                h = (acc + bias).astype(BF)
                if fin is None:
                    o_ref[0, pl.ds(r0, R)] = h.reshape(R, wh, 2 * C)
                    s1, s2 = stats_of(h)
                    t1 = t1 + (s1[:, :C] + s1[:, C:])
                    t2 = t2 + (s2[:, :C] + s2[:, C:])
                else:
                    v = u_ref[0, pl.ds(r0, R)].reshape(R * wh, 2 * C).astype(F32) + h.astype(F32)
                    T[pl.ds(0, R * wh, stride=2), :] = v[:, :C]
                    T[pl.ds(1, R * wh, stride=2), :] = v[:, C:]
                    o_ref[0, pl.ds(r0, R)] = T[...].astype(BF).reshape(R, 2 * wh, C)
            if fin is None:
                if weight0:
                    drop = jnp.logical_and(first, step == 2)
                    t1 = jnp.where(drop, 0.0, t1)
                    t2 = jnp.where(drop, 0.0, t2)
                st_ref[0:1] += t1
                st_ref[1:2] += t2

    def full(shape):
        return pl.BlockSpec(shape, lambda i: (0,) * len(shape))
    fb = (1, hh, wh, 2 * C)
    specs = [pl.BlockSpec(fb, functools.partial(lambda m, i: (m(i), 0, 0, 0), m)) for _, m in ins]
    specs += [full((2, C)), full((1, C)), full((1, C)), full((27, C, C)), full((1, C))]
    args = [a for a, _ in ins] + [s, g, be, w, b]
    scratch = [pltpu.VMEM((ring, hh + 2, wh, 4 * C), BF), pltpu.VMEM((9, 4 * C, 2 * C), BF)]
    alias = {}
    if fin is None:
        out_shape = [jax.ShapeDtypeStruct((nf, hh, wh, 2 * C), BF), jax.ShapeDtypeStruct((2, C), F32)]
        out_specs = [pl.BlockSpec(fb, lambda i: (jnp.maximum(i - 2, 0), 0, 0, 0)), full((2, C))]
    else:
        u, u0, y = fin
        specs.append(pl.BlockSpec(fb, lambda i: (jnp.maximum(i - 2, 0) + u0, 0, 0, 0)))
        args.append(u)
        if y is not None:
            specs.append(pl.BlockSpec(memory_space=pl.ANY))
            alias = {len(args): 0}
            args.append(y)
        scratch.append(pltpu.VMEM((2 * R * wh, C), F32))
        out_shape = jax.ShapeDtypeStruct((4, hh, 2 * wh, C), BF)
        out_specs = pl.BlockSpec((1, hh, 2 * wh, C), lambda i: (jnp.maximum(i - 2, 0) + out_from, 0, 0, 0))
    return pl.pallas_call(
        kern, grid=(nf + 2,), in_specs=specs, out_specs=out_specs, out_shape=out_shape, scratch_shapes=scratch, input_output_aliases=alias,
        compiler_params=pltpu.CompilerParams(dimension_semantics=('arbitrary',), vmem_limit_bytes=VMEM_LIMIT), cost_estimate=cost(nf * 7e9), name='conv_b')(*args)


def solution(mesh):
    nt = mesh.shape['t']
    perm = [(i, i + 1) for i in range(nt - 1)]
    groups = (8, nt // 8)

    def shift_t(x):
        return lax.ppermute(x, 't', perm)

    def local(z, w, b, gamma, beta):
        n, hh, ww, c = z.shape
        wf = [w[i].reshape(27, C, C) for i in range(5)]
        row = lambda a, i: a[i:i + 1]
        cnt1 = float(nt * n * hh * ww * 4)
        cnt2 = float((nt * 2 * n - 1) * 4 * hh * ww * 4)
        zh = shift_t(z)
        s0 = all_reduce([z_stats(z)], groups, 0)
        h, p = conv_a(z, zh, s0, row(gamma, 0), row(beta, 0), wf[0], row(b, 0), cnt1)
        hh_ = shift_t(h)
        s1 = all_reduce([p], groups, 1)
        x = conv_a(h, hh_, s1, row(gamma, 1), row(beta, 1), wf[1], row(b, 1), cnt1, res=z)
        u, p = up_conv(x, shift_t(x), wf[2], row(b, 2))
        s2 = all_reduce([p], groups, 2)
        a3 = (s2, row(gamma, 2), row(beta, 2), wf[3], row(b, 3), cnt2)
        hi, p1 = conv_b([(u, lambda i: i + 2)], *a3, 0, 2)
        hal = shift_t(hi)
        lo, p0 = conv_b([(u, lambda i: i)], *a3, 0, 2, weight0=True)
        s3 = all_reduce([p0, p1], groups, 3)
        a4 = (s3, row(gamma, 3), row(beta, 3), wf[4], row(b, 4), cnt2)
        before = lambda i: jnp.minimum(i, 1)
        after = lambda i: jnp.maximum(i - 2, 0)
        y = conv_b([(lo, before), (hi, after)], *a4, 2, 2, fin=(u, 4, None))
        y = conv_b([(hal, before), (lo, after)], *a4, 0, 2, fin=(u, 2, y), halo=True)
        return y

    spec = P(('batch', 't'))
    return jax.shard_map(local, mesh=mesh, in_specs=(spec, P(), P(), P(), P()), out_specs=spec, check_vma=False)
```

```python
import jax
import jax.numpy as jnp
from jax import lax
from jax.experimental import pallas as pl
from jax.experimental.pallas import tpu as pltpu
from jax.sharding import PartitionSpec as P

F32, BF = jnp.float32, jnp.bfloat16
EPS = 1e-6
C = 128
C2, C3, C4 = 2 * C, 3 * C, 4 * C
ALL, LOW, HIGH, MID = slice(0, C2), slice(0, C), slice(C, C2), slice(C, C3)
TAPS = range(3)
PAIR = range(2)
MESH = pl.DeviceIdType.MESH
R = 8


def dup(v):
    return jnp.concatenate([v, v], axis=1)


def dot(a, b):
    return jnp.dot(a, b, preferred_element_type=F32)


def plus(a, b):
    return b if a is None else a + b


def group_sum(s):
    lane = lax.broadcasted_iota(jnp.int32, s.shape, 1) % 4
    out = s
    for k in (1, 2, 3):
        out = out + jnp.where(lane + k < 4, pltpu.roll(s, C - k, 1), pltpu.roll(s, 4 - k, 1))
    return out


def norm_rows(s, cnt):
    s = group_sum(s)
    mean = s[0:1] / cnt
    return mean, lax.rsqrt(s[1:2] / cnt - mean * mean + EPS)


def act(x, mean, inv, g, be):
    v = (((x.astype(F32) - mean) * inv) * g + be).astype(BF).astype(F32)
    return v * jax.nn.sigmoid(v)


def shift(v, by):
    n = v.shape[0]
    row = lax.broadcasted_iota(jnp.int32, v.shape, 0)
    return jnp.where(row == (0 if by > 0 else n - 1), 0.0, pltpu.roll(v, by % n, 0))


def stats_of(h):
    hf = h.astype(F32)
    return jnp.sum(hf, axis=0, keepdims=True), jnp.sum(hf * hf, axis=0, keepdims=True)


class Net:
    def __init__(self, n, slots0, slots1, cur, ssem, rsem):
        self.n, self.slots, self.cur, self.ssem, self.rsem = n, (slots0, slots1), cur, ssem, rsem
        self.groups = (8, n // 8)
        self.strides = (1, 8)
        self.me = lax.axis_index('t')
        self.next = lax.rem(self.me + 1, n)
        self.prev = lax.rem(self.me + n - 1, n)

    @staticmethod
    def scratch(n, nsum):
        dma = pltpu.SemaphoreType.DMA((nsum, 2))
        return [pltpu.VMEM((nsum, g, 2, C), F32) for g in (8, n // 8)] + [pltpu.VMEM((nsum, 2, 2, C), F32), dma, dma]

    def peer(self, k, i):
        g, st = self.groups[k], self.strides[k]
        d = lax.rem(lax.div(self.me, st), g)
        return self.me + (lax.rem(d + i, g) - d) * st, d

    def greet(self):
        bar = pltpu.get_barrier_semaphore()
        peers = [self.peer(k, i)[0] for k in PAIR for i in range(1, self.groups[k])]
        for d in peers + [self.next, self.prev]:
            pl.semaphore_signal(bar, inc=1, device_id={'t': d}, device_id_type=MESH)

    def met(self):
        pl.semaphore_wait(pltpu.get_barrier_semaphore(), sum(self.groups))

    def send(self, src, dst, ssem, rsem):
        cp = pltpu.make_async_remote_copy(src, dst, ssem, rsem, device_id={'t': self.next}, device_id_type=MESH)
        cp.start()
        return cp

    def total(self, j, v, meanwhile=None, between=None):
        for k in PAIR:
            g = self.groups[k]
            buf = self.slots[k]
            d = self.peer(k, 0)[1]
            self.cur[j, k] = v
            buf[j, pl.ds(d, 1)] = v[None]
            for i in range(1, g):
                pltpu.make_async_remote_copy(self.cur.at[j, k], buf.at[j, d], self.ssem.at[j, k], self.rsem.at[j, k], device_id={'t': self.peer(k, i)[0]}, device_id_type=MESH).start()
            if k == 0 and meanwhile is not None:
                meanwhile()
            w = buf.at[j, pl.ds(0, g - 1)]
            pltpu.make_async_copy(w, w, self.rsem.at[j, k]).wait()
            v = jnp.sum(buf[j], axis=0)
            if k == 0 and between is not None:
                between()
        return v

    def close(self, j):
        for k in PAIR:
            w = self.slots[k].at[j, pl.ds(0, self.groups[k] - 1)]
            pltpu.make_async_copy(w, w, self.ssem.at[j, k]).wait()


def section(z, w, b, gamma, beta, nt, cnt1, cnt2):
    n, hh, ww, _ = z.shape
    wp = ww + 16
    half = hh // 2
    h2 = 2 * hh
    own = 2 * n
    nu = own + 2
    SUB = 2

    def kern(z_ref, w_ref, b_ref, g_ref, be_ref, y_ref, wv, h, hal, x, xhal, U, H, Hh, st, wsem, hs, hr, bs, br, *net):
        nw = Net(nt, *net)
        nw.greet()
        wcp = [pltpu.make_async_copy(w_ref.at[pl.ds(27 * i, 27)], wv.at[i], wsem.at[i]) for i in range(5)]
        for cp in wcp:
            cp.start()
        first = nw.me == 0
        zero = jnp.zeros((1, C), F32)
        zcc = jnp.zeros((C, C), BF)
        sends = []

        def keep(t):
            st[0:1] = t[0]
            st[1:2] = t[1]
            return st[...]

        def phase_a(A, W, X, Wpp, Wpc, Wcp, Wcc, PP, PC, CP, CC, Q):
            def zbody(i, c):
                a, d = stats_of(z_ref[i // hh, i % hh])
                return c[0] + a, c[1] + d
            zs = lax.fori_loop(0, n * hh, zbody, (zero, zero))

            def build(i):
                wcp[i].wait()
                for q in range(4):
                    for di in TAPS:
                        for dj in TAPS:
                            t = di * 3 + dj
                            rows = pl.ds(dj * C, C)
                            W[q * 3 + di, rows, LOW] = wv[i, q * 9 + t] if q < 3 else zcc
                            W[q * 3 + di, rows, HIGH] = wv[i, (q - 1) * 9 + t] if q > 0 else zcc

            def halo(k, src, dst):
                sends.append(nw.send(src, dst, hs.at[k], hr.at[k]))

            def conv(i, src, mine, tot, emit):
                mean, inv = norm_rows(tot, cnt1)
                gg, bb = g_ref[i:i + 1], be_ref[i:i + 1]

                def fill(q):
                    A[q, 0] = jnp.zeros((ww, C3), BF)
                    A[q, hh + 1] = jnp.zeros((ww, C3), BF)

                    def arow(r, c):
                        v = mine[q - 2, r] if q >= 2 else jnp.where(first, mine[0, r], src[q, r])
                        v = act(v, mean, inv, gg, bb)
                        A[q, r + 1, :, HIGH] = v.astype(BF)
                        A[q, r + 1, :, LOW] = shift(v, 1).astype(BF)
                        A[q, r + 1, :, C2:C3] = shift(v, -1).astype(BF)
                        return c
                    lax.fori_loop(0, hh, arow, 0, unroll=2)
                fill(2)
                fill(3)
                sends[-1].wait_recv()
                fill(0)
                fill(1)
                bias = dup(b_ref[i:i + 1])
                for rc in range(hh // R):
                    parts = [A[q, pl.ds(rc * R + di, R)].reshape(R * ww, C3) for q in range(4) for di in TAPS]
                    acc = dot(jnp.concatenate(parts, axis=1), W[...].reshape(12 * C3, C2))
                    emit(pl.ds(rc * R, R), (acc + bias).astype(BF), rc)

            nw.met()
            tot = nw.total(0, keep(zs), lambda: build(0), lambda: halo(0, z_ref, hal.at[0]))
            part = []

            def emit0(rows, v, rc):
                for f in PAIR:
                    h[f, rows] = v[:, f * C:(f + 1) * C].reshape(R, ww, C)
                part.append([a[:, LOW] + a[:, HIGH] for a in stats_of(v)])
            conv(0, hal.at[0], z_ref, tot, emit0)
            tot = nw.total(1, keep([sum(p) for p in zip(*part)]), lambda: build(1), lambda: halo(1, h, hal.at[1]))

            def emit1(rows, v, rc):
                for f in PAIR:
                    x[f, rows] = (z_ref[f, rows].astype(F32) + v[:, f * C:(f + 1) * C].reshape(R, ww, C).astype(F32)).astype(BF)
                halo(2 + rc, x.at[:, rows], xhal.at[:, rows])
            conv(1, hal.at[1], h, tot, emit1)

            wcp[2].wait()

            def put(Wd, k, t):
                for ti in PAIR:
                    Wd[ti, pl.ds(k * C, C), LOW] = wv[2, 18 * ti + t]
                    Wd[ti, pl.ds(k * C, C), HIGH] = wv[2, 9 + t] if ti else zcc
            for Wd, ts in ((Wpp, (0, 2, 6, 8)), (Wpc, (1, 7)), (Wcp, (3, 5)), (Wcc, (4,))):
                for k, t in enumerate(ts):
                    put(Wd, k, t)
            bias = b_ref[2:3]

            def place(q):
                X[q, 0] = jnp.zeros((wp, C2), BF)
                X[q, hh + 1] = jnp.zeros((wp, C2), BF)

                def xrow(r, c):
                    v = x[q - 2, r] if q >= 2 else jnp.where(first, x[0, r], xhal[q, r])
                    X[q, r + 1, 0:ww, HIGH] = v
                    X[q, r + 1, ww:wp, HIGH] = jnp.zeros((16, C), BF)
                    vf = v.astype(F32)
                    X[q, r + 1, 0:ww, LOW] = shift(vf, 1).astype(BF)
                    tail = jnp.where(lax.broadcasted_iota(jnp.int32, (16, C), 0) == 0, vf[ww - 1:ww], 0.0)
                    X[q, r + 1, ww:wp, LOW] = tail.astype(BF)
                    return c
                lax.fori_loop(0, hh, xrow, 0, unroll=2)

            def frame(q, full):
                frames = (q - 1, q) if full else (q,)

                def part_dot(D, Wd, rows, r0, nr, cols):
                    wd = ww if cols else wp
                    parts = [X[f, pl.ds(r0 + dr, nr), 0:wd, cols:C2].reshape(nr * wd, C2 - cols) for f in frames for dr in rows]
                    wt = Wd[...].reshape(2 * Wd.shape[1], C2) if full else Wd[1]
                    D[pl.ds(r0, nr)] = dot(jnp.concatenate(parts, axis=1), wt).reshape(nr, wd, C2)

                for r0, nr in ((0, half), (half, half + 1)):
                    part_dot(PP, Wpp, (0, 1), r0, nr, 0)
                    part_dot(PC, Wpc, (0, 1), r0, nr, C)
                for r0 in (0, half):
                    part_dot(CP, Wcp, (1,), r0, half, 0)
                    part_dot(CC, Wcc, (1,), r0, half, C)
                lanes = ALL if full else HIGH

                def comb(i, c):
                    cp, cc = CP[i, :, lanes], CC[i, :, lanes]
                    c = list(c)
                    for pr in PAIR:
                        fp = PP[i + pr, :, lanes] + cp
                        fc = PC[i + pr, :, lanes] + cc
                        for pc in PAIR:
                            v = (pltpu.roll(fp, wp - 1, 0) if pc else fp)[0:ww] + fc
                            if full:
                                for e, t in enumerate((Q[pr, pc, i], v[:, HIGH])):
                                    o = ((v[:, LOW] + t) + bias).astype(BF)
                                    U[2 * q - 2 + e, 2 * i + pr, :, pc * C:(pc + 1) * C] = o
                                    if q >= 2:
                                        a, d = stats_of(o)
                                        c[2 * e], c[2 * e + 1] = c[2 * e] + a, c[2 * e + 1] + d
                            Q[pr, pc, i] = v[:, HIGH] if full else v
                    return tuple(c)
                c = lax.fori_loop(0, hh, comb, (zero,) * 4)
                drop = jnp.logical_and(first, q == 2)
                return [jnp.where(drop, 0.0, c[k]) + c[2 + k] for k in PAIR]

            place(2)
            place(3)
            frame(2, False)
            sums = frame(3, True)
            for cp in sends[2:]:
                cp.wait_recv()
            place(0)
            place(1)
            frame(0, False)
            frame(1, True)
            keep([a + d for a, d in zip(sums, frame(2, True))])
            for cp in sends:
                cp.wait_send()
            for j in PAIR:
                nw.close(j)

        def phase_b(A0, A1, A2, A3, A4, A5, W, WE, WO, T, Y, ysem):
            A = (A0, A1, A2, A3, A4, A5)

            def build(i):
                wcp[i].wait()
                for t in range(9):
                    for a in PAIR:
                        for o in PAIR:
                            W[t, a * C:(a + 1) * C, o * C:(o + 1) * C] = wv[i, t * 3 + a - o + 1]
                for k in TAPS:
                    for p in range(4):
                        for o in PAIR:
                            t = (k * 3 + p - o) * 3
                            for Wx, dj in ((WE, 0), (WO, 2)):
                                Wx[k * 4 + p, :, o * C:(o + 1) * C] = wv[i, t + dj] if 0 <= p - o <= 2 else zcc

            def prep():
                build(3)
                for a in A:
                    a[0] = jnp.zeros((ww, C4), BF)
                    a[h2 + 1] = jnp.zeros((ww, C4), BF)

            def filler(i, tot, src):
                mean, inv = norm_rows(tot, cnt2)
                mean, inv, gg, bb = dup(mean), dup(inv), dup(g_ref[i - 1:i]), dup(be_ref[i - 1:i])

                def row(k, r):
                    v = act(src(k, r), mean, inv, gg, bb)
                    a = A[k]
                    a[r + 1, :, MID] = v.astype(BF)
                    a[r + 1, :, LOW] = shift(v[:, HIGH], 1).astype(BF)
                    a[r + 1, :, C3:C4] = shift(v[:, LOW], -1).astype(BF)
                return row

            def fill(row, ks):
                def body(r, c):
                    for k in ks:
                        row(k, r)
                    return c
                lax.fori_loop(0, h2, body, 0, unroll=2)

            def conv(i, f, row, ks, emit):
                bias = b_ref[i:i + 1]

                def trip(j, c):
                    for s in range(SUB):
                        r0 = j * (SUB * R) + s * R
                        todo = [(k, r0 + q) for q in range(R) for k in ks]
                        step = -(-len(todo) // 15)

                        def some():
                            for _ in range(step):
                                if todo:
                                    row(*todo.pop(0))
                        acc = None
                        left = [None, None]
                        for k in TAPS:
                            a = A[f + k]
                            for di in TAPS:
                                acc = plus(acc, dot(a[pl.ds(r0 + di, R), :, MID].reshape(R * ww, C2), W[k * 3 + di]))
                                some()
                            for e, (Wx, l0) in enumerate(((WE, 0), (WO, C3))):
                                lhs = [jnp.concatenate([a[r0 + p + q, :, l0:l0 + C] for q in range(0, R, 2)], axis=0) for p in range(4)]
                                left[e] = plus(left[e], dot(jnp.concatenate(lhs, axis=1), Wx[k * 4:k * 4 + 4].reshape(C4, C2)))
                                some()
                        while todo:
                            some()
                        for q in range(R):
                            m = acc[q * ww:(q + 1) * ww]
                            lr = slice(q // 2 * ww, (q // 2 + 1) * ww)
                            lc = slice(q % 2 * C, (q % 2 + 1) * C)
                            c = emit(r0 + q, q, [(m[:, hf] + left[e][lr, lc] + bias).astype(BF) for e, hf in enumerate((LOW, HIGH))], c)
                    return c
                return lambda done=None: lax.fori_loop(0, h2 // (SUB * R), trip if done is None else lambda j, c: done(j, trip(j, c)), (zero, zero))

            def conv3(f, row, ks):
                def emit(r, q, v, c):
                    H[f, r, :, LOW], H[f, r, :, HIGH] = v
                    v = [a.astype(F32) for a in v]
                    return c[0] + jnp.sum(v[0] + v[1], axis=0, keepdims=True), c[1] + jnp.sum(v[0] * v[0] + v[1] * v[1], axis=0, keepdims=True)
                return conv(3, f, row, ks, emit)()

            def conv4(f, row, ks):
                slot = f % 2

                def emit(r, q, v, c):
                    for e, hf in enumerate((LOW, HIGH)):
                        T[pl.ds(q * 2 * ww + e, ww, stride=2), :] = U[f + 2, r, :, hf].astype(F32) + v[e].astype(F32)
                    Y[slot, r] = T[q * 2 * ww:(q + 1) * 2 * ww].astype(BF)
                    return c

                def done(j, c):
                    rows = pl.ds(j * (SUB * R), SUB * R)
                    pltpu.make_async_copy(Y.at[slot, rows], y_ref.at[f, rows], ysem.at[slot]).start()
                    return c
                conv(4, f, row, ks, emit)(done)
                return pltpu.make_async_copy(Y.at[slot], y_ref.at[f], ysem.at[slot])

            row = filler(3, nw.total(2, st[...], prep), lambda k, r: U[k, r])
            fill(row, (2, 3, 4))
            sums = [conv3(2, row, (5,))]
            big = [nw.send(H.at[2], Hh.at[0], bs.at[0], br.at[0])]
            sums.append(conv3(3, row, (0, 1)))
            t0 = conv3(0, row, ())
            sums.append([jnp.where(first, 0.0, a) for a in t0])
            sums.append(conv3(1, row, ()))
            tot = nw.total(3, keep([sum(p) for p in zip(*sums)]), lambda: build(4), lambda: big.append(nw.send(H.at[3], Hh.at[1], bs.at[1], br.at[1])))

            row = filler(4, tot, lambda k, r: H[k - 2, r] if k >= 2 else jnp.where(first, H[0, r], Hh[k, r]))
            fill(row, (2, 3, 4))
            y2 = conv4(2, row, (5,))
            big[0].wait_recv()
            y3 = conv4(3, row, (0,))
            big[1].wait_recv()
            fill(row, (1,))
            y2.wait()
            y0 = conv4(0, row, ())
            y3.wait()
            y1 = conv4(1, row, ())
            for cp in big:
                cp.wait_send()
            for j in (2, 3):
                nw.close(j)
            y0.wait()
            y1.wait()

        V = pltpu.VMEM
        pl.run_scoped(
            phase_a, V((4, hh + 2, ww, C3), BF), V((12, C3, C2), BF), V((4, hh + 2, wp, C2), BF),
            *[V((2, k * C, C2), BF) for k in (4, 2, 2, 1)],
            V((hh + 1, wp, C2), F32), V((hh + 1, ww, C2), F32), V((hh, wp, C2), F32), V((hh, ww, C2), F32), V((2, 2, hh, ww, C), F32))
        pl.run_scoped(
            phase_b, *[V((h2 + 2, ww, C4), BF) for _ in range(nu)], V((9, C2, C2), BF), V((12, C, C2), BF), V((12, C, C2), BF),
            V((2 * R * ww, C), F32), V((2, h2, 2 * ww, C), BF), pltpu.SemaphoreType.DMA((2,)))

    vm = pl.BlockSpec(memory_space=pltpu.VMEM)
    hbm = pl.BlockSpec(memory_space=pl.ANY)
    V, D = pltpu.VMEM, pltpu.SemaphoreType.DMA
    nh = 2 + hh // R
    wide = (h2, ww, C2)
    return pl.pallas_call(
        kern, in_specs=[vm, hbm, vm, vm, vm], out_specs=hbm,
        out_shape=jax.ShapeDtypeStruct((own, h2, 2 * ww, C), BF),
        scratch_shapes=[
            V((5, 27, C, C), BF), V(z.shape, BF), V((2,) + z.shape, BF), V(z.shape, BF), V(z.shape, BF),
            V((nu,) + wide, BF), V((own,) + wide, BF), V((2,) + wide, BF), V((2, C), F32),
            D((5,)), D((nh,)), D((nh,)), D((2,)), D((2,))] + Net.scratch(nt, 4),
        compiler_params=pltpu.CompilerParams(collective_id=0, has_side_effects=True, vmem_limit_bytes=63 * 2**20), name='section')(z, w, b, gamma, beta)


def solution(mesh):
    nt = mesh.shape['t']

    def local(z, w, b, gamma, beta):
        n, hh, ww, c = z.shape
        cnt1 = float(nt * n * hh * ww * 4)
        cnt2 = float((nt * 2 * n - 1) * 4 * hh * ww * 4)
        return section(z, w.reshape(5 * 27, C, C), b, gamma, beta, nt, cnt1, cnt2)

    spec = P(('batch', 't'))
    return jax.shard_map(local, mesh=mesh, in_specs=(spec, P(), P(), P(), P()), out_specs=spec, check_vma=False)
```

```python
import jax
import jax.numpy as jnp
from jax import lax
from jax.experimental import pallas as pl
from jax.experimental.pallas import tpu as pltpu
from jax.sharding import PartitionSpec as P

F32, BF = jnp.float32, jnp.bfloat16
EPS = 1e-6
C = 128
C2, C3, C4 = 2 * C, 3 * C, 4 * C
ALL, LOW, HIGH, MID = slice(0, C2), slice(0, C), slice(C, C2), slice(C, C3)
TAPS = range(3)
PAIR = range(2)
MESH = pl.DeviceIdType.MESH
R = 8


def dup(v):
    return jnp.concatenate([v, v], axis=1)


def dot(a, b):
    return jnp.dot(a, b, preferred_element_type=F32)


def plus(a, b):
    return b if a is None else a + b


def group_sum(s):
    lane = lax.broadcasted_iota(jnp.int32, s.shape, 1) % 4
    out = s
    for k in (1, 2, 3):
        out = out + jnp.where(lane + k < 4, pltpu.roll(s, C - k, 1), pltpu.roll(s, 4 - k, 1))
    return out


def norm_rows(s, cnt):
    s = group_sum(s)
    mean = s[0:1] / cnt
    return mean, lax.rsqrt(s[1:2] / cnt - mean * mean + EPS)


def act(x, mean, inv, g, be):
    v = (((x.astype(F32) - mean) * inv) * g + be).astype(BF).astype(F32)
    return v * jax.nn.sigmoid(v)


def shift(v, by):
    n = v.shape[0]
    row = lax.broadcasted_iota(jnp.int32, v.shape, 0)
    return jnp.where(row == (0 if by > 0 else n - 1), 0.0, pltpu.roll(v, by % n, 0))


def stats_of(h):
    hf = h.astype(F32)
    return jnp.sum(hf, axis=0, keepdims=True), jnp.sum(hf * hf, axis=0, keepdims=True)


class Net:
    def __init__(self, n, slots0, slots1, cur, ssem, rsem):
        self.n, self.slots, self.cur, self.ssem, self.rsem = n, (slots0, slots1), cur, ssem, rsem
        self.groups = (8, n // 8)
        self.strides = (1, 8)
        self.me = lax.axis_index('t')
        self.next = lax.rem(self.me + 1, n)
        self.prev = lax.rem(self.me + n - 1, n)

    @staticmethod
    def scratch(n, nsum):
        dma = pltpu.SemaphoreType.DMA((nsum, 2))
        return [pltpu.VMEM((nsum, g, 2, C), F32) for g in (8, n // 8)] + [pltpu.VMEM((nsum, 2, 2, C), F32), dma, dma]

    def peer(self, k, i):
        g, st = self.groups[k], self.strides[k]
        d = lax.rem(lax.div(self.me, st), g)
        return self.me + (lax.rem(d + i, g) - d) * st, d

    def greet(self):
        bar = pltpu.get_barrier_semaphore()
        peers = [self.peer(k, i)[0] for k in PAIR for i in range(1, self.groups[k])]
        for d in peers + [self.next, self.prev]:
            pl.semaphore_signal(bar, inc=1, device_id={'t': d}, device_id_type=MESH)

    def met(self):
        pl.semaphore_wait(pltpu.get_barrier_semaphore(), sum(self.groups))

    def send(self, src, dst, ssem, rsem):
        cp = pltpu.make_async_remote_copy(src, dst, ssem, rsem, device_id={'t': self.next}, device_id_type=MESH)
        cp.start()
        return cp

    def total(self, j, v, *after):
        for k in PAIR:
            g = self.groups[k]
            buf = self.slots[k]
            d = self.peer(k, 0)[1]
            self.cur[j, k] = v
            buf[j, pl.ds(d, 1)] = v[None]
            for i in range(1, g):
                pltpu.make_async_remote_copy(self.cur.at[j, k], buf.at[j, d], self.ssem.at[j, k], self.rsem.at[j, k], device_id={'t': self.peer(k, i)[0]}, device_id_type=MESH).start()
            if k == 0:
                for job in after:
                    job()
            w = buf.at[j, pl.ds(0, g - 1)]
            pltpu.make_async_copy(w, w, self.rsem.at[j, k]).wait()
            v = jnp.sum(buf[j], axis=0)
        return v

    def close(self, j):
        for k in PAIR:
            w = self.slots[k].at[j, pl.ds(0, self.groups[k] - 1)]
            pltpu.make_async_copy(w, w, self.ssem.at[j, k]).wait()


def section(z, w, b, gamma, beta, nt, cnt1, cnt2):
    n, hh, ww, _ = z.shape
    wp = ww + 16
    half = hh // 2
    h2 = 2 * hh
    own = 2 * n
    nu = own + 2
    SUB = 2

    def kern(z_ref, w_ref, b_ref, g_ref, be_ref, y_ref, wv, h, hal, x, xhal, U, H, Hh, st, wsem, hs, hr, bs, br, *net):
        nw = Net(nt, *net)
        nw.greet()
        wcp = [pltpu.make_async_copy(w_ref.at[pl.ds(27 * i, 27)], wv.at[i], wsem.at[i]) for i in range(5)]
        for cp in wcp:
            cp.start()
        first = nw.me == 0
        zero = jnp.zeros((1, C), F32)
        zcc = jnp.zeros((C, C), BF)
        sends = []

        def keep(t):
            st[0:1] = t[0]
            st[1:2] = t[1]
            return st[...]

        def phase_a(A, W, X, Wpp, Wpc, Wcp, Wcc, PP, PC, CP, CC, Q):
            def zbody(i, c):
                a, d = stats_of(z_ref[i // hh, i % hh])
                return c[0] + a, c[1] + d
            zs = lax.fori_loop(0, n * hh, zbody, (zero, zero))

            def build(i):
                wcp[i].wait()
                for q in range(4):
                    for di in TAPS:
                        for dj in TAPS:
                            t = di * 3 + dj
                            rows = pl.ds(dj * C, C)
                            W[q * 3 + di, rows, LOW] = wv[i, q * 9 + t] if q < 3 else zcc
                            W[q * 3 + di, rows, HIGH] = wv[i, (q - 1) * 9 + t] if q > 0 else zcc

            def halo(k, src, dst):
                sends.append(nw.send(src, dst, hs.at[k], hr.at[k]))

            def conv(i, src, mine, tot, emit):
                mean, inv = norm_rows(tot, cnt1)
                gg, bb = g_ref[i:i + 1], be_ref[i:i + 1]

                def fill(q):
                    A[q, 0] = jnp.zeros((ww, C3), BF)
                    A[q, hh + 1] = jnp.zeros((ww, C3), BF)

                    def arow(r, c):
                        v = mine[q - 2, r] if q >= 2 else jnp.where(first, mine[0, r], src[q, r])
                        v = act(v, mean, inv, gg, bb)
                        A[q, r + 1, :, HIGH] = v.astype(BF)
                        A[q, r + 1, :, LOW] = shift(v, 1).astype(BF)
                        A[q, r + 1, :, C2:C3] = shift(v, -1).astype(BF)
                        return c
                    lax.fori_loop(0, hh, arow, 0, unroll=2)
                fill(2)
                fill(3)
                sends[-1].wait_recv()
                fill(0)
                fill(1)
                bias = dup(b_ref[i:i + 1])
                for rc in range(hh // R):
                    parts = [A[q, pl.ds(rc * R + di, R)].reshape(R * ww, C3) for q in range(4) for di in TAPS]
                    acc = dot(jnp.concatenate(parts, axis=1), W[...].reshape(12 * C3, C2))
                    emit(pl.ds(rc * R, R), (acc + bias).astype(BF), rc)

            nw.met()
            tot = nw.total(0, keep(zs), lambda: halo(0, z_ref, hal.at[0]), lambda: build(0))
            part = []

            def emit0(rows, v, rc):
                for f in PAIR:
                    h[f, rows] = v[:, f * C:(f + 1) * C].reshape(R, ww, C)
                part.append([a[:, LOW] + a[:, HIGH] for a in stats_of(v)])
            conv(0, hal.at[0], z_ref, tot, emit0)
            tot = nw.total(1, keep([sum(p) for p in zip(*part)]), lambda: halo(1, h, hal.at[1]), lambda: build(1))

            def emit1(rows, v, rc):
                for f in PAIR:
                    x[f, rows] = (z_ref[f, rows].astype(F32) + v[:, f * C:(f + 1) * C].reshape(R, ww, C).astype(F32)).astype(BF)
                halo(2 + rc, x.at[:, rows], xhal.at[:, rows])
            conv(1, hal.at[1], h, tot, emit1)

            wcp[2].wait()

            def put(Wd, k, t):
                for ti in PAIR:
                    Wd[ti, pl.ds(k * C, C), LOW] = wv[2, 18 * ti + t]
                    Wd[ti, pl.ds(k * C, C), HIGH] = wv[2, 9 + t] if ti else zcc
            for Wd, ts in ((Wpp, (0, 2, 6, 8)), (Wpc, (1, 7)), (Wcp, (3, 5)), (Wcc, (4,))):
                for k, t in enumerate(ts):
                    put(Wd, k, t)
            bias = b_ref[2:3]

            def place(q):
                X[q, 0] = jnp.zeros((wp, C2), BF)
                X[q, hh + 1] = jnp.zeros((wp, C2), BF)

                def xrow(r, c):
                    v = x[q - 2, r] if q >= 2 else jnp.where(first, x[0, r], xhal[q, r])
                    X[q, r + 1, 0:ww, HIGH] = v
                    X[q, r + 1, ww:wp, HIGH] = jnp.zeros((16, C), BF)
                    vf = v.astype(F32)
                    X[q, r + 1, 0:ww, LOW] = shift(vf, 1).astype(BF)
                    tail = jnp.where(lax.broadcasted_iota(jnp.int32, (16, C), 0) == 0, vf[ww - 1:ww], 0.0)
                    X[q, r + 1, ww:wp, LOW] = tail.astype(BF)
                    return c
                lax.fori_loop(0, hh, xrow, 0, unroll=2)

            def frame(q, full):
                frames = (q - 1, q) if full else (q,)

                def part_dot(D, Wd, rows, r0, nr, cols):
                    wd = ww if cols else wp
                    parts = [X[f, pl.ds(r0 + dr, nr), 0:wd, cols:C2].reshape(nr * wd, C2 - cols) for f in frames for dr in rows]
                    wt = Wd[...].reshape(2 * Wd.shape[1], C2) if full else Wd[1]
                    D[pl.ds(r0, nr)] = dot(jnp.concatenate(parts, axis=1), wt).reshape(nr, wd, C2)

                for r0, nr in ((0, half), (half, half + 1)):
                    part_dot(PP, Wpp, (0, 1), r0, nr, 0)
                    part_dot(PC, Wpc, (0, 1), r0, nr, C)
                for r0 in (0, half):
                    part_dot(CP, Wcp, (1,), r0, half, 0)
                    part_dot(CC, Wcc, (1,), r0, half, C)
                lanes = ALL if full else HIGH

                def comb(i, c):
                    cp, cc = CP[i, :, lanes], CC[i, :, lanes]
                    c = list(c)
                    for pr in PAIR:
                        fp = PP[i + pr, :, lanes] + cp
                        fc = PC[i + pr, :, lanes] + cc
                        for pc in PAIR:
                            v = (pltpu.roll(fp, wp - 1, 0) if pc else fp)[0:ww] + fc
                            if full:
                                for e, t in enumerate((Q[pr, pc, i], v[:, HIGH])):
                                    o = ((v[:, LOW] + t) + bias).astype(BF)
                                    U[2 * q - 2 + e, 2 * i + pr, :, pc * C:(pc + 1) * C] = o
                                    a, d = stats_of(o)
                                    c[2 * e], c[2 * e + 1] = c[2 * e] + a, c[2 * e + 1] + d
                            Q[pr, pc, i] = v[:, HIGH] if full else v
                    return tuple(c)
                c = lax.fori_loop(0, hh, comb, (zero,) * 4)
                drop = jnp.logical_and(first, q == 2)
                return [jnp.where(drop, 0.0, c[k]) + c[2 + k] for k in PAIR]

            place(2)
            place(3)
            frame(2, False)
            sums = frame(3, True)
            for cp in sends[2:]:
                cp.wait_recv()
            place(0)
            place(1)
            frame(0, False)
            own0 = lax.fori_loop(1, 3, lambda q, c: tuple(frame(q, True)), (zero, zero))
            keep([a + d for a, d in zip(sums, own0)])
            for cp in sends:
                cp.wait_send()
            for j in PAIR:
                nw.close(j)

        def phase_b(A0, A1, A2, A3, A4, A5, W, WE, WO, T, Y, ysem):
            A = (A0, A1, A2, A3, A4, A5)

            def build(i):
                wcp[i].wait()
                for t in range(9):
                    for a in PAIR:
                        for o in PAIR:
                            W[t, a * C:(a + 1) * C, o * C:(o + 1) * C] = wv[i, t * 3 + a - o + 1]
                for k in TAPS:
                    for p in range(4):
                        for o in PAIR:
                            t = (k * 3 + p - o) * 3
                            for Wx, dj in ((WE, 0), (WO, 2)):
                                Wx[k * 4 + p, :, o * C:(o + 1) * C] = wv[i, t + dj] if 0 <= p - o <= 2 else zcc

            def prep():
                build(3)
                for a in A:
                    a[0] = jnp.zeros((ww, C4), BF)
                    a[h2 + 1] = jnp.zeros((ww, C4), BF)

            def filler(i, tot, src):
                mean, inv = norm_rows(tot, cnt2)
                mean, inv, gg, bb = dup(mean), dup(inv), dup(g_ref[i - 1:i]), dup(be_ref[i - 1:i])

                def row(k, r):
                    v = act(src(k, r), mean, inv, gg, bb)
                    a = A[k]
                    a[r + 1, :, MID] = v.astype(BF)
                    a[r + 1, :, LOW] = shift(v[:, HIGH], 1).astype(BF)
                    a[r + 1, :, C3:C4] = shift(v[:, LOW], -1).astype(BF)
                return row

            def fill(row, ks):
                def body(r, c):
                    for k in ks:
                        row(k, r)
                    return c
                lax.fori_loop(0, h2, body, 0)

            def conv(i, f, row, ks, emit, done):
                bias = b_ref[i:i + 1]

                def trip(j, c):
                    for s in range(SUB):
                        r0 = j * (SUB * R) + s * R
                        todo = [(k, r0 + q) for q in range(R) for k in ks]
                        step = -(-len(todo) // 15)

                        def some():
                            for _ in range(step):
                                if todo:
                                    row(*todo.pop(0))
                        acc = None
                        left = [None, None]
                        for k in TAPS:
                            a = A[f + k]
                            for di in TAPS:
                                acc = plus(acc, dot(a[pl.ds(r0 + di, R), :, MID].reshape(R * ww, C2), W[k * 3 + di]))
                                some()
                            for e, (Wx, l0) in enumerate(((WE, 0), (WO, C3))):
                                lhs = [jnp.concatenate([a[r0 + p + q, :, l0:l0 + C] for q in range(0, R, 2)], axis=0) for p in range(4)]
                                left[e] = plus(left[e], dot(jnp.concatenate(lhs, axis=1), Wx[k * 4:k * 4 + 4].reshape(C4, C2)))
                                some()
                        while todo:
                            some()
                        for q in range(R):
                            m = acc[q * ww:(q + 1) * ww]
                            lr = slice(q // 2 * ww, (q // 2 + 1) * ww)
                            lc = slice(q % 2 * C, (q % 2 + 1) * C)
                            c = emit(r0 + q, q, [(m[:, hf] + left[e][lr, lc] + bias).astype(BF) for e, hf in enumerate((LOW, HIGH))], c)
                    return done(j, c)
                return lax.fori_loop(0, h2 // (SUB * R), trip, (zero, zero))

            def conv3(f, row, ks, send=None):
                def emit(r, q, v, c):
                    H[f, r, :, LOW], H[f, r, :, HIGH] = v
                    v = [a.astype(F32) for a in v]
                    return c[0] + jnp.sum(v[0] + v[1], axis=0, keepdims=True), c[1] + jnp.sum(v[0] * v[0] + v[1] * v[1], axis=0, keepdims=True)

                def done(j, c):
                    if send is not None:
                        send(pl.ds(j * (SUB * R), SUB * R))
                    return c
                return conv(3, f, row, ks, emit, done)

            def conv4(f, row, ks):
                slot = f % 2

                def emit(r, q, v, c):
                    for e, hf in enumerate((LOW, HIGH)):
                        T[pl.ds(q * 2 * ww + e, ww, stride=2), :] = U[f + 2, r, :, hf].astype(F32) + v[e].astype(F32)
                    Y[slot, r] = T[q * 2 * ww:(q + 1) * 2 * ww].astype(BF)
                    return c

                def done(j, c):
                    rows = pl.ds(j * (SUB * R), SUB * R)
                    pltpu.make_async_copy(Y.at[slot, rows], y_ref.at[f, rows], ysem.at[slot]).start()
                    return c
                conv(4, f, row, ks, emit, done)
                return pltpu.make_async_copy(Y.at[slot], y_ref.at[f], ysem.at[slot])

            row = filler(3, nw.total(2, st[...], prep), lambda k, r: U[k, r])
            fill(row, (3, 4, 5))
            big = [pltpu.make_async_remote_copy(H.at[f], Hh.at[f - 2], bs.at[f - 2], br.at[f - 2], device_id={'t': nw.next}, device_id_type=MESH) for f in (2, 3)]
            sums = [conv3(3, row, (2,), lambda rows: nw.send(H.at[3, rows], Hh.at[1, rows], bs.at[1], br.at[1]))]
            sums.append(conv3(2, row, (1,)))
            sums.append(conv3(1, row, (0,)))
            sums.append([jnp.where(first, 0.0, a) for a in conv3(0, row, ())])
            tot = nw.total(3, keep([sum(p) for p in zip(*sums)]), lambda: build(4))
            big[0].start()

            row = filler(4, tot, lambda k, r: H[k - 2, r] if k >= 2 else jnp.where(first, H[0, r], Hh[k, r]))
            fill(row, (3, 4, 5))
            y3 = conv4(3, row, (2,))
            big[1].wait_recv()
            y2 = conv4(2, row, (1,))
            y3.wait()
            y1 = conv4(1, row, ())
            y2.wait()
            big[0].wait_recv()
            fill(row, (0,))
            y0 = conv4(0, row, ())
            for cp in big:
                cp.wait_send()
            for j in (2, 3):
                nw.close(j)
            y0.wait()
            y1.wait()

        V = pltpu.VMEM
        pl.run_scoped(
            phase_a, V((4, hh + 2, ww, C3), BF), V((12, C3, C2), BF), V((4, hh + 2, wp, C2), BF),
            *[V((2, k * C, C2), BF) for k in (4, 2, 2, 1)],
            V((hh + 1, wp, C2), F32), V((hh + 1, ww, C2), F32), V((hh, wp, C2), F32), V((hh, ww, C2), F32), V((2, 2, hh, ww, C), F32))
        pl.run_scoped(
            phase_b, *[V((h2 + 2, ww, C4), BF) for _ in range(nu)], V((9, C2, C2), BF), V((12, C, C2), BF), V((12, C, C2), BF),
            V((2 * R * ww, C), F32), V((2, h2, 2 * ww, C), BF), pltpu.SemaphoreType.DMA((2,)))

    vm = pl.BlockSpec(memory_space=pltpu.VMEM)
    hbm = pl.BlockSpec(memory_space=pl.ANY)
    V, D = pltpu.VMEM, pltpu.SemaphoreType.DMA
    nh = 2 + hh // R
    wide = (h2, ww, C2)
    return pl.pallas_call(
        kern, in_specs=[vm, hbm, vm, vm, vm], out_specs=hbm,
        out_shape=jax.ShapeDtypeStruct((own, h2, 2 * ww, C), BF),
        scratch_shapes=[
            V((5, 27, C, C), BF), V(z.shape, BF), V((2,) + z.shape, BF), V(z.shape, BF), V(z.shape, BF),
            V((nu,) + wide, BF), V((own,) + wide, BF), V((2,) + wide, BF), V((2, C), F32),
            D((5,)), D((nh,)), D((nh,)), D((2,)), D((2,))] + Net.scratch(nt, 4),
        compiler_params=pltpu.CompilerParams(collective_id=0, has_side_effects=True, vmem_limit_bytes=63 * 2**20), name='section')(z, w, b, gamma, beta)


def solution(mesh):
    nt = mesh.shape['t']

    def local(z, w, b, gamma, beta):
        n, hh, ww, c = z.shape
        cnt1 = float(nt * n * hh * ww * 4)
        cnt2 = float((nt * 2 * n - 1) * 4 * hh * ww * 4)
        return section(z, w.reshape(5 * 27, C, C), b, gamma, beta, nt, cnt1, cnt2)

    spec = P(('batch', 't'))
    return jax.shard_map(local, mesh=mesh, in_specs=(spec, P(), P(), P(), P()), out_specs=spec, check_vma=False)
```

```python
import jax
import jax.numpy as jnp
from jax import lax
from jax.experimental import pallas as pl
from jax.experimental.pallas import tpu as pltpu
from jax.sharding import PartitionSpec as P

F32, BF = jnp.float32, jnp.bfloat16
EPS = 1e-6
C = 128
C2, C3, C4 = 2 * C, 3 * C, 4 * C
ALL, LOW, HIGH, MID = slice(0, C2), slice(0, C), slice(C, C2), slice(C, C3)
TAPS = range(3)
PAIR = range(2)
MESH = pl.DeviceIdType.MESH
R = 8


def dup(v):
    return jnp.concatenate([v, v], axis=1)


def dot(a, b):
    return jnp.dot(a, b, preferred_element_type=F32)


def plus(a, b):
    return b if a is None else a + b


def group_sum(s):
    lane = lax.broadcasted_iota(jnp.int32, s.shape, 1) % 4
    out = s
    for k in (1, 2, 3):
        out = out + jnp.where(lane + k < 4, pltpu.roll(s, C - k, 1), pltpu.roll(s, 4 - k, 1))
    return out


def norm_rows(s, cnt):
    s = group_sum(s)
    mean = s[0:1] / cnt
    return mean, lax.rsqrt(s[1:2] / cnt - mean * mean + EPS)


def act(x, mean, inv, g, be):
    v = (((x.astype(F32) - mean) * inv) * g + be).astype(BF).astype(F32)
    return v * jax.nn.sigmoid(v)


def shift(v, by):
    n = v.shape[0]
    row = lax.broadcasted_iota(jnp.int32, v.shape, 0)
    return jnp.where(row == (0 if by > 0 else n - 1), 0.0, pltpu.roll(v, by % n, 0))


def stats_of(h):
    hf = h.astype(F32)
    return jnp.sum(hf, axis=0, keepdims=True), jnp.sum(hf * hf, axis=0, keepdims=True)


class Net:
    def __init__(self, n, slots0, slots1, cur, ssem, rsem):
        self.n, self.slots, self.cur, self.ssem, self.rsem = n, (slots0, slots1), cur, ssem, rsem
        self.groups = (8, n // 8)
        self.strides = (1, 8)
        self.me = lax.axis_index('t')
        self.next = lax.rem(self.me + 1, n)
        self.prev = lax.rem(self.me + n - 1, n)

    @staticmethod
    def scratch(n, nsum):
        dma = pltpu.SemaphoreType.DMA((nsum, 2))
        return [pltpu.VMEM((nsum, g, 2, C), F32) for g in (8, n // 8)] + [pltpu.VMEM((nsum, 2, 2, C), F32), dma, dma]

    def peer(self, k, i):
        g, st = self.groups[k], self.strides[k]
        d = lax.rem(lax.div(self.me, st), g)
        return self.me + (lax.rem(d + i, g) - d) * st, d

    def greet(self):
        bar = pltpu.get_barrier_semaphore()
        peers = [self.peer(k, i)[0] for k in PAIR for i in range(1, self.groups[k])]
        for d in peers + [self.next, self.prev]:
            pl.semaphore_signal(bar, inc=1, device_id={'t': d}, device_id_type=MESH)

    def met(self):
        pl.semaphore_wait(pltpu.get_barrier_semaphore(), sum(self.groups))

    def send(self, src, dst, ssem, rsem):
        cp = pltpu.make_async_remote_copy(src, dst, ssem, rsem, device_id={'t': self.next}, device_id_type=MESH)
        cp.start()
        return cp

    def total(self, j, v, *after):
        for k in PAIR:
            g = self.groups[k]
            buf = self.slots[k]
            d = self.peer(k, 0)[1]
            self.cur[j, k] = v
            buf[j, pl.ds(d, 1)] = v[None]
            for i in range(1, g):
                pltpu.make_async_remote_copy(self.cur.at[j, k], buf.at[j, d], self.ssem.at[j, k], self.rsem.at[j, k], device_id={'t': self.peer(k, i)[0]}, device_id_type=MESH).start()
            if k == 0:
                for job in after:
                    job()
            w = buf.at[j, pl.ds(0, g - 1)]
            pltpu.make_async_copy(w, w, self.rsem.at[j, k]).wait()
            v = jnp.sum(buf[j], axis=0)
        return v

    def close(self, j):
        for k in PAIR:
            w = self.slots[k].at[j, pl.ds(0, self.groups[k] - 1)]
            pltpu.make_async_copy(w, w, self.ssem.at[j, k]).wait()


def section(z, w, b, gamma, beta, nt, cnt1, cnt2):
    n, hh, ww, _ = z.shape
    wp = ww + 16
    half = hh // 2
    h2 = 2 * hh
    own = 2 * n
    nu = own + 2
    SUB = 2

    def kern(z_ref, w_ref, b_ref, g_ref, be_ref, y_ref, wv, h, hal, x, xhal, U, H, Hh, st, wsem, hs, hr, bs, br, *net):
        nw = Net(nt, *net)
        nw.greet()
        wcp = [pltpu.make_async_copy(w_ref.at[pl.ds(27 * i, 27)], wv.at[i], wsem.at[i]) for i in range(5)]
        for cp in wcp:
            cp.start()
        first = nw.me == 0
        zero = jnp.zeros((1, C), F32)
        zcc = jnp.zeros((C, C), BF)
        sends = []

        def keep(t):
            st[0:1] = t[0]
            st[1:2] = t[1]
            return st[...]

        def phase_a(A, W, X, Wpp, Wpc, Wcp, Wcc, PP, PC, CP, CC, Q):
            def zbody(i, c):
                a, d = stats_of(z_ref[i // hh, i % hh])
                return c[0] + a, c[1] + d
            zs = lax.fori_loop(0, n * hh, zbody, (zero, zero))

            def build(i):
                wcp[i].wait()
                for q in range(4):
                    for di in TAPS:
                        for dj in TAPS:
                            t = di * 3 + dj
                            rows = pl.ds(dj * C, C)
                            W[q * 3 + di, rows, LOW] = wv[i, q * 9 + t] if q < 3 else zcc
                            W[q * 3 + di, rows, HIGH] = wv[i, (q - 1) * 9 + t] if q > 0 else zcc

            def halo(k, src, dst):
                sends.append(nw.send(src, dst, hs.at[k], hr.at[k]))

            def conv(i, src, mine, tot, emit):
                mean, inv = norm_rows(tot, cnt1)
                gg, bb = g_ref[i:i + 1], be_ref[i:i + 1]

                def fill(q):
                    A[q, 0] = jnp.zeros((ww, C3), BF)
                    A[q, hh + 1] = jnp.zeros((ww, C3), BF)

                    def arow(r, c):
                        v = mine[q - 2, r] if q >= 2 else jnp.where(first, mine[0, r], src[q, r])
                        v = act(v, mean, inv, gg, bb)
                        A[q, r + 1, :, HIGH] = v.astype(BF)
                        A[q, r + 1, :, LOW] = shift(v, 1).astype(BF)
                        A[q, r + 1, :, C2:C3] = shift(v, -1).astype(BF)
                        return c
                    lax.fori_loop(0, hh, arow, 0, unroll=2)
                fill(2)
                fill(3)
                sends[-1].wait_recv()
                fill(0)
                fill(1)
                bias = dup(b_ref[i:i + 1])
                for rc in range(hh // R):
                    parts = [A[q, pl.ds(rc * R + di, R)].reshape(R * ww, C3) for q in range(4) for di in TAPS]
                    acc = dot(jnp.concatenate(parts, axis=1), W[...].reshape(12 * C3, C2))
                    emit(pl.ds(rc * R, R), (acc + bias).astype(BF), rc)

            nw.met()
            tot = nw.total(0, keep(zs), lambda: halo(0, z_ref, hal.at[0]), lambda: build(0))
            part = []

            def emit0(rows, v, rc):
                for f in PAIR:
                    h[f, rows] = v[:, f * C:(f + 1) * C].reshape(R, ww, C)
                part.append([a[:, LOW] + a[:, HIGH] for a in stats_of(v)])
            conv(0, hal.at[0], z_ref, tot, emit0)
            tot = nw.total(1, keep([sum(p) for p in zip(*part)]), lambda: halo(1, h, hal.at[1]), lambda: build(1))

            def emit1(rows, v, rc):
                for f in PAIR:
                    x[f, rows] = (z_ref[f, rows].astype(F32) + v[:, f * C:(f + 1) * C].reshape(R, ww, C).astype(F32)).astype(BF)
                halo(2 + rc, x.at[:, rows], xhal.at[:, rows])
            conv(1, hal.at[1], h, tot, emit1)

            wcp[2].wait()

            def put(Wd, k, t):
                for ti in PAIR:
                    Wd[ti, pl.ds(k * C, C), LOW] = wv[2, 18 * ti + t]
                    Wd[ti, pl.ds(k * C, C), HIGH] = wv[2, 9 + t] if ti else zcc
            for Wd, ts in ((Wpp, (0, 2, 6, 8)), (Wpc, (1, 7)), (Wcp, (3, 5)), (Wcc, (4,))):
                for k, t in enumerate(ts):
                    put(Wd, k, t)
            bias = b_ref[2:3]

            def place(q):
                X[q, 0] = jnp.zeros((wp, C2), BF)
                X[q, hh + 1] = jnp.zeros((wp, C2), BF)

                def xrow(r, c):
                    v = x[q - 2, r] if q >= 2 else jnp.where(first, x[0, r], xhal[q, r])
                    X[q, r + 1, 0:ww, HIGH] = v
                    X[q, r + 1, ww:wp, HIGH] = jnp.zeros((16, C), BF)
                    vf = v.astype(F32)
                    X[q, r + 1, 0:ww, LOW] = shift(vf, 1).astype(BF)
                    tail = jnp.where(lax.broadcasted_iota(jnp.int32, (16, C), 0) == 0, vf[ww - 1:ww], 0.0)
                    X[q, r + 1, ww:wp, LOW] = tail.astype(BF)
                    return c
                lax.fori_loop(0, hh, xrow, 0, unroll=2)

            def frame(q, full):
                frames = (q - 1, q) if full else (q,)

                def part_dot(D, Wd, rows, r0, nr, cols):
                    wd = ww if cols else wp
                    parts = [X[f, pl.ds(r0 + dr, nr), 0:wd, cols:C2].reshape(nr * wd, C2 - cols) for f in frames for dr in rows]
                    wt = Wd[...].reshape(2 * Wd.shape[1], C2) if full else Wd[1]
                    D[pl.ds(r0, nr)] = dot(jnp.concatenate(parts, axis=1), wt).reshape(nr, wd, C2)

                for r0, nr in ((0, half), (half, half + 1)):
                    part_dot(PP, Wpp, (0, 1), r0, nr, 0)
                    part_dot(PC, Wpc, (0, 1), r0, nr, C)
                for r0 in (0, half):
                    part_dot(CP, Wcp, (1,), r0, half, 0)
                    part_dot(CC, Wcc, (1,), r0, half, C)
                lanes = ALL if full else HIGH

                def comb(i, c):
                    cp, cc = CP[i, :, lanes], CC[i, :, lanes]
                    c = list(c)
                    for pr in PAIR:
                        fp = PP[i + pr, :, lanes] + cp
                        fc = PC[i + pr, :, lanes] + cc
                        for pc in PAIR:
                            v = (pltpu.roll(fp, wp - 1, 0) if pc else fp)[0:ww] + fc
                            if full:
                                for e, t in enumerate((Q[pr, pc, i], v[:, HIGH])):
                                    o = ((v[:, LOW] + t) + bias).astype(BF)
                                    U[2 * q - 2 + e, 2 * i + pr, :, pc * C:(pc + 1) * C] = o
                                    a, d = stats_of(o)
                                    c[2 * e], c[2 * e + 1] = c[2 * e] + a, c[2 * e + 1] + d
                            Q[pr, pc, i] = v[:, HIGH] if full else v
                    return tuple(c)
                c = lax.fori_loop(0, hh, comb, (zero,) * 4)
                drop = jnp.logical_and(first, q == 2)
                return [jnp.where(drop, 0.0, c[k]) + c[2 + k] for k in PAIR]

            place(2)
            place(3)
            frame(2, False)
            sums = frame(3, True)
            for cp in sends[2:]:
                cp.wait_recv()
            place(0)
            place(1)
            frame(0, False)
            own0 = lax.fori_loop(1, 3, lambda q, c: tuple(frame(q, True)), (zero, zero))
            keep([a + d for a, d in zip(sums, own0)])
            for cp in sends:
                cp.wait_send()
            for j in PAIR:
                nw.close(j)

        def phase_b(A0, A1, A2, A3, A4, A5, W, WE, WO, T):
            A = (A0, A1, A2, A3, A4, A5)

            def build(i):
                wcp[i].wait()
                for t in range(9):
                    for a in PAIR:
                        for o in PAIR:
                            W[t, a * C:(a + 1) * C, o * C:(o + 1) * C] = wv[i, t * 3 + a - o + 1]
                for k in TAPS:
                    for p in range(4):
                        for o in PAIR:
                            t = (k * 3 + p - o) * 3
                            for Wx, dj in ((WE, 0), (WO, 2)):
                                Wx[k * 4 + p, :, o * C:(o + 1) * C] = wv[i, t + dj] if 0 <= p - o <= 2 else zcc

            def prep():
                build(3)
                for a in A:
                    a[0] = jnp.zeros((ww, C4), BF)
                    a[h2 + 1] = jnp.zeros((ww, C4), BF)

            def filler(i, tot, src):
                mean, inv = norm_rows(tot, cnt2)
                mean, inv, gg, bb = dup(mean), dup(inv), dup(g_ref[i - 1:i]), dup(be_ref[i - 1:i])

                def row(k, r):
                    v = act(src(k, r), mean, inv, gg, bb)
                    a = A[k]
                    a[r + 1, :, MID] = v.astype(BF)
                    a[r + 1, :, LOW] = shift(v[:, HIGH], 1).astype(BF)
                    a[r + 1, :, C3:C4] = shift(v[:, LOW], -1).astype(BF)
                return row

            def fill(row, ks):
                def body(r, c):
                    for k in ks:
                        row(k, r)
                    return c
                lax.fori_loop(0, h2, body, 0)

            def conv(i, f, row, ks, emit, done):
                bias = b_ref[i:i + 1]

                def trip(j, c):
                    for s in range(SUB):
                        r0 = j * (SUB * R) + s * R
                        todo = [(k, r0 + q) for q in range(R) for k in ks]
                        step = -(-len(todo) // 15)

                        def some():
                            for _ in range(step):
                                if todo:
                                    row(*todo.pop(0))
                        acc = None
                        left = [None, None]
                        for k in TAPS:
                            a = A[f + k]
                            for di in TAPS:
                                acc = plus(acc, dot(a[pl.ds(r0 + di, R), :, MID].reshape(R * ww, C2), W[k * 3 + di]))
                                some()
                            for e, (Wx, l0) in enumerate(((WE, 0), (WO, C3))):
                                lhs = [jnp.concatenate([a[r0 + p + q, :, l0:l0 + C] for q in range(0, R, 2)], axis=0) for p in range(4)]
                                left[e] = plus(left[e], dot(jnp.concatenate(lhs, axis=1), Wx[k * 4:k * 4 + 4].reshape(C4, C2)))
                                some()
                        while todo:
                            some()
                        for q in range(R):
                            m = acc[q * ww:(q + 1) * ww]
                            lr = slice(q // 2 * ww, (q // 2 + 1) * ww)
                            lc = slice(q % 2 * C, (q % 2 + 1) * C)
                            c = emit(r0 + q, q, [(m[:, hf] + left[e][lr, lc] + bias).astype(BF) for e, hf in enumerate((LOW, HIGH))], c)
                    return done(j, c)
                return lax.fori_loop(0, h2 // (SUB * R), trip, (zero, zero))

            def conv3(f, row, ks, send=None):
                def emit(r, q, v, c):
                    H[f, r, :, LOW], H[f, r, :, HIGH] = v
                    v = [a.astype(F32) for a in v]
                    return c[0] + jnp.sum(v[0] + v[1], axis=0, keepdims=True), c[1] + jnp.sum(v[0] * v[0] + v[1] * v[1], axis=0, keepdims=True)

                def done(j, c):
                    if send is not None:
                        send(pl.ds(j * (SUB * R), SUB * R))
                    return c
                return conv(3, f, row, ks, emit, done)

            def conv4(f, row, ks):

                def emit(r, q, v, c):
                    for e, hf in enumerate((LOW, HIGH)):
                        T[pl.ds(q * 2 * ww + e, ww, stride=2), :] = U[f + 2, r, :, hf].astype(F32) + v[e].astype(F32)
                    y_ref[f, r] = T[q * 2 * ww:(q + 1) * 2 * ww].astype(BF)
                    return c

                conv(4, f, row, ks, emit, lambda j, c: c)

            row = filler(3, nw.total(2, st[...], prep), lambda k, r: U[k, r])
            fill(row, (3, 4, 5))
            big = [pltpu.make_async_remote_copy(H.at[f], Hh.at[f - 2], bs.at[f - 2], br.at[f - 2], device_id={'t': nw.next}, device_id_type=MESH) for f in (2, 3)]
            sums = [conv3(3, row, (2,), lambda rows: nw.send(H.at[3, rows], Hh.at[1, rows], bs.at[1], br.at[1]))]
            sums.append(conv3(2, row, (1,)))
            sums.append(conv3(1, row, (0,)))
            sums.append([jnp.where(first, 0.0, a) for a in conv3(0, row, ())])
            tot = nw.total(3, keep([sum(p) for p in zip(*sums)]), lambda: build(4))
            big[0].start()

            row = filler(4, tot, lambda k, r: H[k - 2, r] if k >= 2 else jnp.where(first, H[0, r], Hh[k, r]))
            fill(row, (3, 4, 5))
            conv4(3, row, (2,))
            big[1].wait_recv()
            conv4(2, row, (1,))
            conv4(1, row, ())
            big[0].wait_recv()
            fill(row, (0,))
            conv4(0, row, ())
            for cp in big:
                cp.wait_send()
            for j in (2, 3):
                nw.close(j)

        V = pltpu.VMEM
        pl.run_scoped(
            phase_a, V((4, hh + 2, ww, C3), BF), V((12, C3, C2), BF), V((4, hh + 2, wp, C2), BF),
            *[V((2, k * C, C2), BF) for k in (4, 2, 2, 1)],
            V((hh + 1, wp, C2), F32), V((hh + 1, ww, C2), F32), V((hh, wp, C2), F32), V((hh, ww, C2), F32), V((2, 2, hh, ww, C), F32))
        pl.run_scoped(
            phase_b, *[V((h2 + 2, ww, C4), BF) for _ in range(nu)], V((9, C2, C2), BF), V((12, C, C2), BF), V((12, C, C2), BF),
            V((2 * R * ww, C), F32))

    vm = pl.BlockSpec(memory_space=pltpu.VMEM)
    hbm = pl.BlockSpec(memory_space=pl.ANY)
    V, D = pltpu.VMEM, pltpu.SemaphoreType.DMA
    nh = 2 + hh // R
    wide = (h2, ww, C2)
    return pl.pallas_call(
        kern, in_specs=[vm, hbm, vm, vm, vm], out_specs=vm,
        out_shape=pltpu.VMEM((own, h2, 2 * ww, C), BF),
        scratch_shapes=[
            V((5, 27, C, C), BF), V(z.shape, BF), V((2,) + z.shape, BF), V(z.shape, BF), V(z.shape, BF),
            V((nu,) + wide, BF), V((own,) + wide, BF), V((2,) + wide, BF), V((2, C), F32),
            D((5,)), D((nh,)), D((nh,)), D((2,)), D((2,))] + Net.scratch(nt, 4),
        compiler_params=pltpu.CompilerParams(collective_id=0, has_side_effects=True, vmem_limit_bytes=55 * 2**20), name='section')(z, w, b, gamma, beta)


def solution(mesh):
    nt = mesh.shape['t']

    def local(z, w, b, gamma, beta):
        n, hh, ww, c = z.shape
        cnt1 = float(nt * n * hh * ww * 4)
        cnt2 = float((nt * 2 * n - 1) * 4 * hh * ww * 4)
        return section(z, w.reshape(5 * 27, C, C), b, gamma, beta, nt, cnt1, cnt2)

    spec = P(('batch', 't'))
    return jax.shard_map(local, mesh=mesh, in_specs=(spec, P(), P(), P(), P()), out_specs=spec, check_vma=False)
```

```python
import jax
import jax.numpy as jnp
from jax import lax
from jax.experimental import pallas as pl
from jax.experimental.pallas import tpu as pltpu
from jax.sharding import PartitionSpec as P

F32, BF = jnp.float32, jnp.bfloat16
EPS = 1e-6
C = 128
C2, C3, C4 = 2 * C, 3 * C, 4 * C
ALL, LOW, HIGH, MID = slice(0, C2), slice(0, C), slice(C, C2), slice(C, C3)
TAPS = range(3)
PAIR = range(2)
MESH = pl.DeviceIdType.MESH
R = 8


def dup(v):
    return jnp.concatenate([v, v], axis=1)


def dot(a, b):
    return jnp.dot(a, b, preferred_element_type=F32)


def plus(a, b):
    return b if a is None else a + b


def group_sum(s):
    lane = lax.broadcasted_iota(jnp.int32, s.shape, 1) % 4
    out = s
    for k in (1, 2, 3):
        out = out + jnp.where(lane + k < 4, pltpu.roll(s, C - k, 1), pltpu.roll(s, 4 - k, 1))
    return out


def norm_rows(s, cnt):
    s = group_sum(s)
    mean = s[0:1] / cnt
    return mean, lax.rsqrt(s[1:2] / cnt - mean * mean + EPS)


def act(x, mean, inv, g, be):
    v = (((x.astype(F32) - mean) * inv) * g + be).astype(BF).astype(F32)
    return v * jax.nn.sigmoid(v)


def shift(v, by):
    n = v.shape[0]
    row = lax.broadcasted_iota(jnp.int32, v.shape, 0)
    return jnp.where(row == (0 if by > 0 else n - 1), 0.0, pltpu.roll(v, by % n, 0))


def stats_of(h):
    hf = h.astype(F32)
    return jnp.sum(hf, axis=0, keepdims=True), jnp.sum(hf * hf, axis=0, keepdims=True)


class Net:
    def __init__(self, n, slots0, slots1, cur, ssem, rsem):
        self.n, self.slots, self.cur, self.ssem, self.rsem = n, (slots0, slots1), cur, ssem, rsem
        self.groups = (8, n // 8)
        self.strides = (1, 8)
        self.me = lax.axis_index('t')
        self.next = lax.rem(self.me + 1, n)
        self.prev = lax.rem(self.me + n - 1, n)

    @staticmethod
    def scratch(n, nsum):
        dma = pltpu.SemaphoreType.DMA((nsum, 2))
        return [pltpu.VMEM((nsum, g, 2, C), F32) for g in (8, n // 8)] + [pltpu.VMEM((nsum, 2, 2, C), F32), dma, dma]

    def peer(self, k, i):
        g, st = self.groups[k], self.strides[k]
        d = lax.rem(lax.div(self.me, st), g)
        return self.me + (lax.rem(d + i, g) - d) * st, d

    def greet(self):
        bar = pltpu.get_barrier_semaphore()
        peers = [self.peer(k, i)[0] for k in PAIR for i in range(1, self.groups[k])]
        for d in peers + [self.next, self.prev]:
            pl.semaphore_signal(bar, inc=1, device_id={'t': d}, device_id_type=MESH)

    def met(self):
        pl.semaphore_wait(pltpu.get_barrier_semaphore(), sum(self.groups))

    def send(self, src, dst, ssem, rsem):
        cp = pltpu.make_async_remote_copy(src, dst, ssem, rsem, device_id={'t': self.next}, device_id_type=MESH)
        cp.start()
        return cp

    def total(self, j, v, *after):
        for k in PAIR:
            g = self.groups[k]
            buf = self.slots[k]
            d = self.peer(k, 0)[1]
            self.cur[j, k] = v
            buf[j, pl.ds(d, 1)] = v[None]
            for i in range(1, g):
                pltpu.make_async_remote_copy(self.cur.at[j, k], buf.at[j, d], self.ssem.at[j, k], self.rsem.at[j, k], device_id={'t': self.peer(k, i)[0]}, device_id_type=MESH).start()
            if k == 0:
                for job in after:
                    job()
            w = buf.at[j, pl.ds(0, g - 1)]
            pltpu.make_async_copy(w, w, self.rsem.at[j, k]).wait()
            v = jnp.sum(buf[j], axis=0)
        return v

    def close(self, j):
        for k in PAIR:
            w = self.slots[k].at[j, pl.ds(0, self.groups[k] - 1)]
            pltpu.make_async_copy(w, w, self.ssem.at[j, k]).wait()


def section(z, w, b, gamma, beta, nt, cnt1, cnt2):
    n, hh, ww, _ = z.shape
    wp = ww + 16
    half = hh // 2
    h2 = 2 * hh
    own = 2 * n
    nu = own + 2
    SUB = 2

    def kern(z_ref, w_ref, b_ref, g_ref, be_ref, y_ref, wv, h, hal, x, xhal, U, H, Hh, st, wsem, hs, hr, bs, br, *net):
        nw = Net(nt, *net)
        nw.greet()
        wcp = [pltpu.make_async_copy(w_ref.at[pl.ds(27 * i, 27)], wv.at[i], wsem.at[i]) for i in range(5)]
        for cp in wcp:
            cp.start()
        first = nw.me == 0
        zero = jnp.zeros((1, C), F32)
        zcc = jnp.zeros((C, C), BF)
        sends = []

        def keep(t):
            st[0:1] = t[0]
            st[1:2] = t[1]
            return st[...]

        def phase_a(A, W, X, Wpp, Wpc, Wcp, Wcc, PP, PC, CP, CC, Q):
            def zbody(i, c):
                a, d = stats_of(z_ref[i // hh, i % hh])
                return c[0] + a, c[1] + d
            zs = lax.fori_loop(0, n * hh, zbody, (zero, zero))

            def build(i):
                wcp[i].wait()
                for q in range(4):
                    for di in TAPS:
                        for dj in TAPS:
                            t = di * 3 + dj
                            rows = pl.ds(dj * C, C)
                            W[q * 3 + di, rows, LOW] = wv[i, q * 9 + t] if q < 3 else zcc
                            W[q * 3 + di, rows, HIGH] = wv[i, (q - 1) * 9 + t] if q > 0 else zcc

            def halo(k, src, dst):
                sends.append(nw.send(src, dst, hs.at[k], hr.at[k]))

            def conv(i, src, mine, tot, emit):
                mean, inv = norm_rows(tot, cnt1)
                gg, bb = g_ref[i:i + 1], be_ref[i:i + 1]

                def fill(q):
                    A[q, 0] = jnp.zeros((ww, C3), BF)
                    A[q, hh + 1] = jnp.zeros((ww, C3), BF)

                    def arow(r, c):
                        v = mine[q - 2, r] if q >= 2 else jnp.where(first, mine[0, r], src[q, r])
                        v = act(v, mean, inv, gg, bb)
                        A[q, r + 1, :, HIGH] = v.astype(BF)
                        A[q, r + 1, :, LOW] = shift(v, 1).astype(BF)
                        A[q, r + 1, :, C2:C3] = shift(v, -1).astype(BF)
                        return c
                    lax.fori_loop(0, hh, arow, 0, unroll=4)
                def taps_of(qs, rc):
                    parts = [A[q, pl.ds(rc * R + di, R)].reshape(R * ww, C3) for q in qs for di in TAPS]
                    return dot(jnp.concatenate(parts, axis=1), W[3 * qs[0]:3 * qs[0] + 6].reshape(6 * C3, C2))
                fill(2)
                fill(3)
                for rc in range(hh // R):
                    CC[pl.ds(rc * R, R)] = taps_of((2, 3), rc).reshape(R, ww, C2)
                sends[-1].wait_recv()
                fill(0)
                fill(1)
                bias = dup(b_ref[i:i + 1])
                for rc in range(hh // R):
                    rows = pl.ds(rc * R, R)
                    acc = CC[rows].reshape(R * ww, C2) + taps_of((0, 1), rc)
                    emit(rows, (acc + bias).astype(BF), rc)

            nw.met()
            tot = nw.total(0, keep(zs), lambda: halo(0, z_ref, hal.at[0]), lambda: build(0))
            part = []

            def emit0(rows, v, rc):
                for f in PAIR:
                    h[f, rows] = v[:, f * C:(f + 1) * C].reshape(R, ww, C)
                part.append([a[:, LOW] + a[:, HIGH] for a in stats_of(v)])
            conv(0, hal.at[0], z_ref, tot, emit0)
            tot = nw.total(1, keep([sum(p) for p in zip(*part)]), lambda: halo(1, h, hal.at[1]), lambda: build(1))

            def emit1(rows, v, rc):
                for f in PAIR:
                    x[f, rows] = (z_ref[f, rows].astype(F32) + v[:, f * C:(f + 1) * C].reshape(R, ww, C).astype(F32)).astype(BF)
                halo(2 + rc, x.at[:, rows], xhal.at[:, rows])
            conv(1, hal.at[1], h, tot, emit1)

            wcp[2].wait()

            def put(Wd, k, t):
                for ti in PAIR:
                    Wd[ti, pl.ds(k * C, C), LOW] = wv[2, 18 * ti + t]
                    Wd[ti, pl.ds(k * C, C), HIGH] = wv[2, 9 + t] if ti else zcc
            for Wd, ts in ((Wpp, (0, 2, 6, 8)), (Wpc, (1, 7)), (Wcp, (3, 5)), (Wcc, (4,))):
                for k, t in enumerate(ts):
                    put(Wd, k, t)
            bias = b_ref[2:3]

            def place(q):
                X[q, 0] = jnp.zeros((wp, C2), BF)
                X[q, hh + 1] = jnp.zeros((wp, C2), BF)

                def xrow(r, c):
                    v = x[q - 2, r] if q >= 2 else jnp.where(first, x[0, r], xhal[q, r])
                    X[q, r + 1, 0:ww, HIGH] = v
                    X[q, r + 1, ww:wp, HIGH] = jnp.zeros((16, C), BF)
                    vf = v.astype(F32)
                    X[q, r + 1, 0:ww, LOW] = shift(vf, 1).astype(BF)
                    tail = jnp.where(lax.broadcasted_iota(jnp.int32, (16, C), 0) == 0, vf[ww - 1:ww], 0.0)
                    X[q, r + 1, ww:wp, LOW] = tail.astype(BF)
                    return c
                lax.fori_loop(0, hh, xrow, 0, unroll=2)

            def frame(q, full):
                frames = (q - 1, q) if full else (q,)

                def part_dot(D, Wd, rows, r0, nr, cols):
                    wd = ww if cols else wp
                    parts = [X[f, pl.ds(r0 + dr, nr), 0:wd, cols:C2].reshape(nr * wd, C2 - cols) for f in frames for dr in rows]
                    wt = Wd[...].reshape(2 * Wd.shape[1], C2) if full else Wd[1]
                    D[pl.ds(r0, nr)] = dot(jnp.concatenate(parts, axis=1), wt).reshape(nr, wd, C2)

                for r0, nr in ((0, half), (half, half + 1)):
                    part_dot(PP, Wpp, (0, 1), r0, nr, 0)
                    part_dot(PC, Wpc, (0, 1), r0, nr, C)
                for r0 in (0, half):
                    part_dot(CP, Wcp, (1,), r0, half, 0)
                    part_dot(CC, Wcc, (1,), r0, half, C)
                lanes = ALL if full else HIGH

                def comb(i, c):
                    cp, cc = CP[i, :, lanes], CC[i, :, lanes]
                    c = list(c)
                    for pr in PAIR:
                        fp = PP[i + pr, :, lanes] + cp
                        fc = PC[i + pr, :, lanes] + cc
                        for pc in PAIR:
                            v = (pltpu.roll(fp, wp - 1, 0) if pc else fp)[0:ww] + fc
                            if full:
                                for e, t in enumerate((Q[pr, pc, i], v[:, HIGH])):
                                    o = ((v[:, LOW] + t) + bias).astype(BF)
                                    U[2 * q - 2 + e, 2 * i + pr, :, pc * C:(pc + 1) * C] = o
                                    a, d = stats_of(o)
                                    c[2 * e], c[2 * e + 1] = c[2 * e] + a, c[2 * e + 1] + d
                            Q[pr, pc, i] = v[:, HIGH] if full else v
                    return tuple(c)
                c = lax.fori_loop(0, hh, comb, (zero,) * 4)
                drop = jnp.logical_and(first, q == 2)
                return [jnp.where(drop, 0.0, c[k]) + c[2 + k] for k in PAIR]

            place(2)
            place(3)
            frame(2, False)
            sums = frame(3, True)
            for cp in sends[2:]:
                cp.wait_recv()
            place(0)
            place(1)
            frame(0, False)
            own0 = lax.fori_loop(1, 3, lambda q, c: tuple(frame(q, True)), (zero, zero))
            keep([a + d for a, d in zip(sums, own0)])
            for cp in sends:
                cp.wait_send()
            for j in PAIR:
                nw.close(j)

        def phase_b(A0, A1, A2, A3, A4, A5, W, WE, WO, T):
            A = (A0, A1, A2, A3, A4, A5)

            def build(i):
                wcp[i].wait()
                for t in range(9):
                    for a in PAIR:
                        for o in PAIR:
                            W[t, a * C:(a + 1) * C, o * C:(o + 1) * C] = wv[i, t * 3 + a - o + 1]
                for k in TAPS:
                    for p in range(4):
                        for o in PAIR:
                            t = (k * 3 + p - o) * 3
                            for Wx, dj in ((WE, 0), (WO, 2)):
                                Wx[k * 4 + p, :, o * C:(o + 1) * C] = wv[i, t + dj] if 0 <= p - o <= 2 else zcc

            def prep():
                build(3)
                for a in A:
                    a[0] = jnp.zeros((ww, C4), BF)
                    a[h2 + 1] = jnp.zeros((ww, C4), BF)

            def filler(i, tot, src):
                mean, inv = norm_rows(tot, cnt2)
                mean, inv, gg, bb = dup(mean), dup(inv), dup(g_ref[i - 1:i]), dup(be_ref[i - 1:i])

                def row(k, r):
                    v = act(src(k, r), mean, inv, gg, bb)
                    a = A[k]
                    a[r + 1, :, MID] = v.astype(BF)
                    a[r + 1, :, LOW] = shift(v[:, HIGH], 1).astype(BF)
                    a[r + 1, :, C3:C4] = shift(v[:, LOW], -1).astype(BF)
                return row

            def fill(row, ks):
                def body(r, c):
                    for k in ks:
                        row(k, r)
                    return c
                lax.fori_loop(0, h2, body, 0, unroll=2)

            def conv(i, f, row, ks, emit, done):
                bias = b_ref[i:i + 1]

                def trip(j, c):
                    for s in range(SUB):
                        r0 = j * (SUB * R) + s * R
                        todo = [(k, r0 + q) for q in range(R) for k in ks]
                        step = -(-len(todo) // 15)

                        def some():
                            for _ in range(step):
                                if todo:
                                    row(*todo.pop(0))
                        acc = None
                        left = [None, None]
                        for k in TAPS:
                            a = A[f + k]
                            for di in TAPS:
                                acc = plus(acc, dot(a[pl.ds(r0 + di, R), :, MID].reshape(R * ww, C2), W[k * 3 + di]))
                                some()
                            for e, (Wx, l0) in enumerate(((WE, 0), (WO, C3))):
                                lhs = [jnp.concatenate([a[r0 + p + q, :, l0:l0 + C] for q in range(0, R, 2)], axis=0) for p in range(4)]
                                left[e] = plus(left[e], dot(jnp.concatenate(lhs, axis=1), Wx[k * 4:k * 4 + 4].reshape(C4, C2)))
                                some()
                        while todo:
                            some()
                        for q in range(R):
                            m = acc[q * ww:(q + 1) * ww]
                            lr = slice(q // 2 * ww, (q // 2 + 1) * ww)
                            lc = slice(q % 2 * C, (q % 2 + 1) * C)
                            c = emit(r0 + q, q, [(m[:, hf] + left[e][lr, lc] + bias).astype(BF) for e, hf in enumerate((LOW, HIGH))], c)
                    return done(j, c)
                return lax.fori_loop(0, h2 // (SUB * R), trip, (zero, zero))

            def conv3(f, row, ks, send=None):
                def emit(r, q, v, c):
                    H[f, r, :, LOW], H[f, r, :, HIGH] = v
                    v = [a.astype(F32) for a in v]
                    return c[0] + jnp.sum(v[0] + v[1], axis=0, keepdims=True), c[1] + jnp.sum(v[0] * v[0] + v[1] * v[1], axis=0, keepdims=True)

                def done(j, c):
                    if send is not None:
                        send(pl.ds(j * (SUB * R), SUB * R))
                    return c
                return conv(3, f, row, ks, emit, done)

            def conv4(f, row, ks):

                def emit(r, q, v, c):
                    for e, hf in enumerate((LOW, HIGH)):
                        T[pl.ds(q * 2 * ww + e, ww, stride=2), :] = U[f + 2, r, :, hf].astype(F32) + v[e].astype(F32)
                    y_ref[f, r] = T[q * 2 * ww:(q + 1) * 2 * ww].astype(BF)
                    return c

                conv(4, f, row, ks, emit, lambda j, c: c)

            row = filler(3, nw.total(2, st[...], prep), lambda k, r: U[k, r])
            fill(row, (3, 4, 5))
            big = [pltpu.make_async_remote_copy(H.at[f], Hh.at[f - 2], bs.at[f - 2], br.at[f - 2], device_id={'t': nw.next}, device_id_type=MESH) for f in (2, 3)]
            sums = [conv3(3, row, (2,), lambda rows: nw.send(H.at[3, rows], Hh.at[1, rows], bs.at[1], br.at[1]))]
            sums.append(conv3(2, row, (1,)))
            sums.append(conv3(1, row, (0,)))
            sums.append([jnp.where(first, 0.0, a) for a in conv3(0, row, ())])
            tot = nw.total(3, keep([sum(p) for p in zip(*sums)]), lambda: build(4))
            big[0].start()

            row = filler(4, tot, lambda k, r: H[k - 2, r] if k >= 2 else jnp.where(first, H[0, r], Hh[k, r]))
            fill(row, (3, 4, 5))
            conv4(3, row, (2,))
            big[1].wait_recv()
            conv4(2, row, (1,))
            conv4(1, row, ())
            big[0].wait_recv()
            fill(row, (0,))
            conv4(0, row, ())
            for cp in big:
                cp.wait_send()
            for j in (2, 3):
                nw.close(j)

        V = pltpu.VMEM
        pl.run_scoped(
            phase_a, V((4, hh + 2, ww, C3), BF), V((12, C3, C2), BF), V((4, hh + 2, wp, C2), BF),
            *[V((2, k * C, C2), BF) for k in (4, 2, 2, 1)],
            V((hh + 1, wp, C2), F32), V((hh + 1, ww, C2), F32), V((hh, wp, C2), F32), V((hh, ww, C2), F32), V((2, 2, hh, ww, C), F32))
        pl.run_scoped(
            phase_b, *[V((h2 + 2, ww, C4), BF) for _ in range(nu)], V((9, C2, C2), BF), V((12, C, C2), BF), V((12, C, C2), BF),
            V((2 * R * ww, C), F32))

    vm = pl.BlockSpec(memory_space=pltpu.VMEM)
    hbm = pl.BlockSpec(memory_space=pl.ANY)
    V, D = pltpu.VMEM, pltpu.SemaphoreType.DMA
    nh = 2 + hh // R
    wide = (h2, ww, C2)
    return pl.pallas_call(
        kern, in_specs=[vm, hbm, vm, vm, vm], out_specs=vm,
        out_shape=pltpu.VMEM((own, h2, 2 * ww, C), BF),
        scratch_shapes=[
            V((5, 27, C, C), BF), V(z.shape, BF), V((2,) + z.shape, BF), V(z.shape, BF), V(z.shape, BF),
            V((nu,) + wide, BF), V((own,) + wide, BF), V((2,) + wide, BF), V((2, C), F32),
            D((5,)), D((nh,)), D((nh,)), D((2,)), D((2,))] + Net.scratch(nt, 4),
        compiler_params=pltpu.CompilerParams(collective_id=0, has_side_effects=True, vmem_limit_bytes=55 * 2**20), name='section')(z, w, b, gamma, beta)


def solution(mesh):
    nt = mesh.shape['t']

    def local(z, w, b, gamma, beta):
        n, hh, ww, c = z.shape
        cnt1 = float(nt * n * hh * ww * 4)
        cnt2 = float((nt * 2 * n - 1) * 4 * hh * ww * 4)
        return section(z, w.reshape(5 * 27, C, C), b, gamma, beta, nt, cnt1, cnt2)

    spec = P(('batch', 't'))
    return jax.shard_map(local, mesh=mesh, in_specs=(spec, P(), P(), P(), P()), out_specs=spec, check_vma=False)
```
